512 devices in a mesh: groups: 2 (over y), expert: 32 (over z, core), mp: 8 (over x).
Axes of the slice: x: 8, y: 2, z: 16, core: 2. Of those that a mesh axis runs over, the one named last changes fastest.
The devices are a block of a 8x8x16 slice.
Arguments:
- tokens_in: bfloat16 [16384, 2048], P(('groups', 'expert'), 'mp'), parts along dimension 0, may hold values from -6 to 6
- out_grad: bfloat16 [16384, 2048], P(('groups', 'expert'), 'mp'), parts along dimension 0, may hold values from -3 to 3
- logits: float32 [16384, 32], P(('groups', 'expert')), parts along dimension 0, may hold values from -6 to 6
- indices: int32 [64, 256], P('groups'), parts along dimension 0, may hold values from 0 to 8191, as said below
- w_in: bfloat16 [32, 2048, 4096], P('expert', None, 'mp'), may hold values from -0.125 to 0.125
- w_out: bfloat16 [32, 4096, 2048], P('expert', 'mp'), may hold values from -0.09375 to 0.09375
- router_w: bfloat16 [2048, 32], P('mp'), may hold values from -0.125 to 0.125
Outputs:
- input_grad: float32 [16384, 2048], P(('groups', 'expert'), 'mp'), parts along dimension 0
- router_grad: float32 [4096, 32], P(('groups', 'mp')), parts along dimension 0
The draws below stay inside these ranges and needn't reach their ends.
There are 2 independent parts, one for each index of `groups`. The reference program is written for one: setup_inputs(seed, part) draws one part's arguments, and reference() takes and returns one part's arrays. A program takes and returns all parts, laid end to end along the dimension named above; an argument that names none is the same for every part. Nothing has to cross between parts.
Inputs may be any that keep to these rules, and one draw needn't show every extreme that they name: `indices`: each expert's row holds 256 different tokens. Of the 256 tokens of one index of the expert axis (rows k * 256 to (k + 1) * 256 - 1), one expert takes at most 16, and every expert takes exactly 16 from some such index.
All inputs are finite; a program needn't handle non-finite values.
Results may differ from the reference program's by a relative error of at most 0.019.
Values may be sent and summed in bfloat16 or wider, within the bound.
No kernel may reach another device: no remote copies, remote signals or barrier semaphores. Data moves between devices by JAX's collectives and lax.ppermute only.
A program may use at most 64 MiB of HBM per device.

```python
import jax
import jax.numpy as jnp
from jax import lax

D = 2048
HIDDEN_SIZE = 4096
CAPACITY = 256
TOK_DEV = 256
EXPERTS = 32
TOKENS = 8192
MOST = 16


def draw_indices(key, part):
    base = jax.random.fold_in(key, 11)
    source_weight = jax.random.randint(jax.random.fold_in(base, 1), (EXPERTS,), 1, 5)
    copies = EXPERTS * MOST
    owner = jnp.arange(copies, dtype=jnp.int32) // MOST
    within = jnp.arange(copies, dtype=jnp.int32) % MOST

    def one_expert(expert_key):
        keys = jax.random.split(expert_key, 3)
        favoured = jax.random.randint(keys[0], (), 0, EXPERTS)
        score = jax.random.randint(keys[1], (copies,), 0, 1024) * source_weight[owner]
        score = score + 8192 * (owner == favoured).astype(jnp.int32)
        score = score * copies + jnp.arange(copies, dtype=jnp.int32)
        unused, picked = lax.top_k(score, CAPACITY)
        shuffle = jax.random.randint(keys[2], (EXPERTS, TOK_DEV), 0, 1 << 20) * TOK_DEV
        shuffle = shuffle + jnp.arange(TOK_DEV, dtype=jnp.int32)[None, :]
        order = jnp.argsort(shuffle, axis=1).astype(jnp.int32)
        picked_owner = owner[picked]
        picked_within = within[picked]
        return picked_owner * TOK_DEV + order[picked_owner, picked_within]
    return jax.vmap(one_expert)(jax.random.split(base, EXPERTS)).astype(jnp.int32)


def steps_of(rng, dims, pieces, least, high):
    gain, own = 1.0, jax.random.fold_in(rng, 6)
    for dim, parts in pieces:
        draws = jnp.exp(jax.random.uniform(jax.random.fold_in(own, dim), (parts,), jnp.float32, least / len(pieces), high / len(pieces)))
        gain = gain * jnp.repeat(draws, dims[dim] // parts).reshape([-1 if axis == dim else 1 for axis in range(len(dims))])
    return gain


def bell_draw(rng, dims, deviation, most, cuts=(), kind=jnp.bfloat16):
    array = deviation * jax.random.normal(rng, dims, jnp.float32)
    if cuts:
        array = array * steps_of(rng, dims, cuts, -0.22, 0.18)
    return jnp.clip(array, -most, most).astype(kind)


def setup_inputs(seed: int = 0, part: int = 0) -> dict:
    key_of = jax.random.split(jax.random.key(seed), 8)
    part_splits = jax.random.split(jax.random.fold_in(key_of[7], part), 8)
    tokens_in = bell_draw(part_splits[0], (TOKENS, D), 1.0, 6.0, ((0, 32), (1, 8)))
    out_grad = bell_draw(part_splits[1], (TOKENS, D), 0.5, 3.0, ((0, 32), (1, 8)))
    logits = bell_draw(part_splits[2], (TOKENS, EXPERTS), 1.5, 6.0, ((0, 32),), jnp.float32)
    indices = draw_indices(jax.random.fold_in(jax.random.fold_in(key_of[7], part), 71), part)
    w_in = bell_draw(key_of[4], (EXPERTS, D, HIDDEN_SIZE), D ** -0.5, 0.125, ((0, 32), (2, 8)))
    w_out = bell_draw(key_of[5], (EXPERTS, HIDDEN_SIZE, D), HIDDEN_SIZE ** -0.5, 0.09375, ((0, 32), (1, 8)))
    router_w = bell_draw(key_of[6], (D, EXPERTS), D ** -0.5, 0.125, ((0, 8),))
    return {"tokens_in": tokens_in, "out_grad": out_grad, "logits": logits, "indices": indices, "w_in": w_in, "w_out": w_out, "router_w": router_w}


inv_root_two = 0.7071067811865476
inv_root_tau = 0.3989422804014327


def gelu_parts(hidden_pre):
    cumulative = 0.5 * (1.0 + lax.erf(hidden_pre * inv_root_two))
    slopes = cumulative + hidden_pre * jnp.exp(-0.5 * hidden_pre * hidden_pre) * inv_root_tau
    return hidden_pre * cumulative, slopes


def reference(tokens_in, out_grad, logits, indices, w_in, w_out, router_w):
    def expert_step(packed):
        chosen_idx, weight_in, weight_out = packed
        rows_x = tokens_in[chosen_idx]
        rows_dy = out_grad[chosen_idx]
        hidden_pre = jnp.dot(rows_x, weight_in, preferred_element_type=jnp.float32)
        hidden_back = lax.dot_general(rows_dy, weight_out, (((1,), (1,)), ((), ())), preferred_element_type=jnp.float32)
        activated, slopes = gelu_parts(hidden_pre)
        gate_vals = jnp.sum(activated * hidden_back, axis=1)
        delta = (hidden_back * slopes).astype(jnp.bfloat16)
        contrib = lax.dot_general(delta, weight_in, (((1,), (1,)), ((), ())), preferred_element_type=jnp.float32)
        return contrib.astype(jnp.bfloat16), gate_vals

    contribs, gate_vals = lax.map(expert_step, (indices, w_in, w_out))
    gate_probs = jax.nn.sigmoid(logits)
    expert_ids = jnp.broadcast_to(jnp.arange(EXPERTS, dtype=jnp.int32)[:, None], indices.shape)
    chosen_gates = gate_probs[indices, expert_ids]
    weighted = chosen_gates[:, :, None] * contribs.astype(jnp.float32)
    input_grad = jnp.zeros((TOKENS, D), jnp.float32).at[indices.reshape(-1)].add(weighted.reshape(-1, D))
    gate_grad = jnp.zeros((TOKENS, EXPERTS), jnp.float32).at[indices, expert_ids].add(gate_vals)
    logit_grad = (gate_probs * (1.0 - gate_probs) * gate_grad).astype(jnp.bfloat16)
    router_dx = lax.dot_general(logit_grad, router_w, (((1,), (1,)), ((), ())), preferred_element_type=jnp.float32)
    input_grad = input_grad + router_dx
    router_grad = lax.dot_general(tokens_in, logit_grad, (((0,), (0,)), ((), ())), preferred_element_type=jnp.float32)
    return input_grad, router_grad
```

```python
import jax
import jax.numpy as jnp
from jax import lax
from jax.sharding import PartitionSpec as P

inv_root_two = 0.7071067811865476
inv_root_tau = 0.3989422804014327
LANES = 128
EXTRA = 8
f32 = jnp.float32
bf16 = jnp.bfloat16


def mm(a, b, contract=((1,), (0,))):
    return lax.dot_general(a, b, (contract, ((), ())), preferred_element_type=f32)


def gelu_parts(hidden_pre):
    cumulative = 0.5 * (1.0 + lax.erf(hidden_pre * inv_root_two))
    slopes = cumulative + hidden_pre * jnp.exp(-0.5 * hidden_pre * hidden_pre) * inv_root_tau
    return (hidden_pre * cumulative, slopes)


def in_parts(v, parts):
    out = []
    for _ in range(parts):
        part = lax.reduce_precision(v, 8, 7)
        out.append(part.astype(bf16))
        v = v - part
    return out


def lane_blocks(x):
    return [x[:, k : k + LANES] for k in range(0, x.shape[1], LANES)]


def pack_source(tokens, grads, logits, indices, here):
    tok, _ = tokens.shape
    experts, capacity = indices.shape
    most = min(tok, 2 * capacity // experts)
    local = indices - here * tok
    token_range = jnp.arange(tok, dtype=jnp.int32)
    member = jnp.any(local[:, :, None] == token_range[None, None, :], axis=1)
    before = (token_range[:, None] < token_range[None, :]).astype(bf16)
    rank = mm(member.astype(bf16), before).astype(jnp.int32)
    rank = jnp.where(member, rank, -1)
    ranks = jnp.arange(most, dtype=jnp.int32)
    hits = rank[:, None, :] == ranks[None, :, None]
    pick = hits.astype(bf16).reshape(experts * most, tok)
    blocks = [
        mm(pick, b).astype(bf16).reshape(experts, most, LANES)
        for b in lane_blocks(tokens) + lane_blocks(grads)
    ]
    probs = jax.nn.sigmoid(logits).T
    slot_probs = jnp.sum(jnp.where(hits, probs[:, None, :], 0.0), axis=2)
    extra = jnp.stack(in_parts(slot_probs, 3), axis=1)
    blocks.append(jnp.pad(extra, ((0, 0), (0, EXTRA - 3), (0, LANES - most))))
    return jnp.concatenate(blocks, axis=1), pick


def compact(recv, own, tok, most):
    sources = recv.shape[0]
    capacity = own.shape[0]
    src = own // tok
    s_range = jnp.arange(sources, dtype=jnp.int32)
    count = jnp.sum((src[:, None] == s_range[None, :]).astype(jnp.int32), axis=0)
    end = jnp.sum(jnp.where(s_range[:, None] <= s_range[None, :], count[:, None], 0), axis=0)
    start = end - count
    slot = jnp.arange(capacity, dtype=jnp.int32)
    of_source = (slot[:, None] >= start[None, :]) & (slot[:, None] < end[None, :])
    within = slot - jnp.sum(jnp.where(of_source, start[None, :], 0), axis=1)
    lanes = jnp.arange(LANES, dtype=jnp.int32)
    n_rows = recv.shape[1] - EXTRA
    ext = recv[:, n_rows : n_rows + 3, :]
    table = mm(of_source.astype(bf16), ext.reshape(sources, 3 * LANES))
    table = sum(lane_blocks(table))
    probs = jnp.sum(jnp.where(lanes[None, :] == within[:, None], table, 0.0), axis=1)
    ranks = jnp.arange(most, dtype=jnp.int32)
    place = jnp.where(ranks[None, :] < count[:, None], start[:, None] + ranks[None, :], -1)
    place = (slot[:, None, None] == place[None, :, :]).astype(bf16)
    place = place.reshape(capacity, sources * most)
    rows = [
        mm(place, recv[:, k : k + most, :].reshape(sources * most, LANES)).astype(bf16)
        for k in range(0, n_rows, most)
    ]
    return jnp.concatenate(rows, axis=1), probs, place


def gathered(x, axis):
    return lax.all_gather(x, axis)


def hidden_part(rows, weight_in, weight_out):
    devices, capacity, both = rows.shape
    cols = both // 2
    xs = jnp.moveaxis(rows[:, :, :cols], 0, 1).reshape(capacity, devices * cols)
    dys = jnp.moveaxis(rows[:, :, cols:], 0, 1).reshape(capacity, devices * cols)
    pre = mm(xs, weight_in)
    back = mm(dys, weight_out, ((1,), (1,)))
    activated, slopes = gelu_parts(pre)
    gates = jnp.sum(activated * back, axis=1)
    delta = (back * slopes).astype(bf16)
    contrib = mm(delta, weight_in, ((1,), (1,))).astype(bf16)
    contrib = contrib.reshape(capacity, devices, cols // LANES, LANES)
    contrib = contrib.transpose(1, 2, 0, 3).reshape(devices, cols // LANES * capacity, LANES)
    extra = jnp.concatenate([p.reshape(capacity // LANES, LANES) for p in in_parts(gates, 3)])
    extra = jnp.pad(extra, ((0, EXTRA - extra.shape[0]), (0, 0)))
    extra = jnp.broadcast_to(extra[None], (devices, *extra.shape))
    return jnp.concatenate([contrib, extra], axis=1)


def combine(parts, probs, own_x, router_col, place, most):
    capacity, cols = own_x.shape
    total = jnp.sum(parts.astype(f32), axis=0)
    blocks = cols // LANES
    extra = total[blocks * capacity :]
    per = capacity // LANES
    gates = (extra[:per] + extra[per : 2 * per] + extra[2 * per : 3 * per]).reshape(capacity)
    logit_grad = (probs * (1.0 - probs) * gates).astype(bf16)
    column = mm(logit_grad[None, :], own_x)
    sources = place.shape[1] // most
    out = []
    for k in range(blocks):
        block = total[k * capacity : (k + 1) * capacity] * probs[:, None]
        block = block + logit_grad.astype(f32)[:, None] * router_col[None, k * LANES : (k + 1) * LANES]
        block = mm(place, block.astype(bf16), ((0,), (0,))).astype(bf16)
        out.append(block.reshape(sources, most, LANES))
    extra = jnp.concatenate([p.reshape(blocks, LANES) for p in in_parts(column[0], 2)])
    extra = jnp.pad(extra, ((0, EXTRA - extra.shape[0]), (0, 0)))
    out.append(jnp.broadcast_to(extra[None], (sources, *extra.shape)))
    return jnp.concatenate(out, axis=1)


def finish(recv, pick, cols, most):
    experts = recv.shape[0]
    blocks = cols // LANES
    rows = [
        recv[:, k * most : (k + 1) * most, :].reshape(experts * most, LANES) for k in range(blocks)
    ]
    input_grad = mm(pick, jnp.concatenate(rows, axis=1), ((0,), (0,)))
    extra = recv[:, blocks * most :, :].astype(f32)
    column = extra[:, :blocks, :] + extra[:, blocks : 2 * blocks, :]
    return input_grad, column.reshape(experts, cols).T


def per_device(tokens_in, out_grad, logits, indices, w_in, w_out, router_w):
    tok, cols = tokens_in.shape
    experts, capacity = indices.shape
    most = min(tok, 2 * capacity // experts)
    here = lax.axis_index("expert")
    own = lax.dynamic_index_in_dim(indices, here, 0, keepdims=False)
    send, pick = pack_source(tokens_in, out_grad, logits, indices, here)
    recv = lax.all_to_all(send, "expert", 0, 0, tiled=True)
    rows, probs, place = compact(recv, own, tok, most)
    parts = hidden_part(gathered(rows, "mp"), w_in[0], w_out[0])
    parts = lax.all_to_all(parts, "mp", 0, 0, tiled=True)
    e_range = jnp.arange(experts, dtype=jnp.int32)
    router_col = jnp.sum(jnp.where(e_range[None, :] == here, router_w.astype(f32), 0.0), axis=1)
    back = combine(parts, probs, rows[:, :cols], router_col, place, most)
    back = lax.all_to_all(back, "expert", 0, 0, tiled=True)
    return finish(back, pick, cols, most)


def solution(mesh):
    return jax.shard_map(
        per_device,
        mesh=mesh,
        in_specs=(
            P(("groups", "expert"), "mp"),
            P(("groups", "expert"), "mp"),
            P(("groups", "expert"), None),
            P("groups", None),
            P("expert", None, "mp"),
            P("expert", "mp", None),
            P("mp", None),
        ),
        out_specs=(P(("groups", "expert"), "mp"), P(("groups", "mp"), None)),
        check_vma=False,
    )
```

```python
import functools

import jax
import jax.numpy as jnp
from jax import lax
from jax.experimental import pallas as pl
from jax.experimental.pallas import tpu as pltpu
from jax.sharding import PartitionSpec as P


inv_root_two = 0.7071067811865476
inv_root_tau = 0.3989422804014327
LANES = 128
EXTRA = 8
f32 = jnp.float32
bf16 = jnp.bfloat16
i32 = jnp.int32


def mm(a, b, contract=((1,), (0,))):
    return lax.dot_general(a, b, (contract, ((), ())), preferred_element_type=f32)


def iota(shape, dim):
    return lax.broadcasted_iota(i32, shape, dim)


def in_parts(v, parts):
    out = []
    for _ in range(parts):
        part = v.astype(bf16).astype(f32)
        out.append(part)
        v = v - part
    return out


def row_to_column(row):
    n = row.shape[1]
    eye = iota((n, n), 0) == iota((n, n), 1)
    return jnp.sum(jnp.where(eye, row, jnp.zeros_like(row)), axis=1, keepdims=True)


def column_to_row(column):
    n = column.shape[0]
    eye = iota((n, n), 0) == iota((n, n), 1)
    return jnp.sum(jnp.where(eye, column, jnp.zeros_like(column)), axis=0, keepdims=True)


def stacked_rows(rows, height):
    count = rows[0].shape[0]
    at = iota((count, height, LANES), 1)
    out = jnp.zeros((count, height, LANES), f32)
    for k, row in enumerate(rows):
        out = jnp.where(at == k, row[:, None, :], out)
    return out


def pack_kernel(here_ref, idx_ref, tok_ref, grad_ref, logit_ref, send_ref, pick_ref):
    experts, capacity = idx_ref.shape
    tok, cols = tok_ref.shape
    most = pick_ref.shape[0] // experts
    local = idx_ref[...] - here_ref[0] * tok
    token = iota((experts, tok), 1)
    member = jnp.zeros((experts, tok), i32)
    for c in range(capacity):
        member = jnp.where(local[:, c : c + 1] == token, 1, member)
    before = (iota((tok, tok), 0) < iota((tok, tok), 1)).astype(f32).astype(bf16)
    rank = mm(member.astype(f32).astype(bf16), before).astype(i32)
    rank = jnp.where(member == 1, rank, -1)
    ranks = iota((most, tok), 0)
    for e in range(experts):
        hit = jnp.where(rank[e : e + 1, :] == ranks, 1.0, 0.0)
        pick_ref[e * most : (e + 1) * most, :] = hit.astype(bf16)
    pick = pick_ref[...]
    at = 0
    for ref in (tok_ref, grad_ref):
        rows = mm(pick, ref[...]).astype(bf16)
        for k in range(0, cols, LANES):
            send_ref[:, at : at + most, :] = rows[:, k : k + LANES].reshape(experts, most, LANES)
            at += most
    probs = jax.nn.sigmoid(logit_ref[...])
    rows = []
    for part in in_parts(probs, 3):
        rows += [part[:, k : k + LANES] for k in range(0, tok, LANES)]
    send_ref[:, at : at + EXTRA, :] = stacked_rows(rows, EXTRA).astype(bf16)


def compact_kernel(own_ref, recv_ref, rows_ref, probs_ref, place_ref):
    sources = recv_ref.shape[0]
    capacity = own_ref.shape[1]
    spread = place_ref.shape[0]
    most = spread // sources
    tok = 2 * LANES
    square = (capacity, capacity)
    own_row = own_ref[...]
    own_col = row_to_column(own_row)
    pos_row = jnp.sum((own_col < own_row).astype(i32), axis=0, keepdims=True)
    token = jnp.sum(jnp.where(pos_row == iota(square, 0), own_row, 0), axis=1, keepdims=True)
    src = token // tok
    local = token - src * tok
    wide = (capacity, LANES)
    start = jnp.sum((own_col < iota(wide, 1) * tok).astype(i32), axis=0, keepdims=True)
    is_src = src == iota(wide, 1)
    first = jnp.sum(jnp.where(is_src, start, 0), axis=1, keepdims=True)
    target = src * most + iota((capacity, 1), 0) - first
    place = jnp.where(target == iota((capacity, spread), 1), 1.0, 0.0).astype(bf16)
    place_ref[...] = jnp.where(
        column_to_row(target) == iota((spread, capacity), 0), 1.0, 0.0
    ).astype(bf16)
    blocks = rows_ref.shape[1] // LANES
    for k in range(blocks):
        block = recv_ref[:, k * most : (k + 1) * most, :].reshape(spread, LANES)
        rows_ref[:, k * LANES : (k + 1) * LANES] = mm(place, block).astype(bf16)
    pick = jnp.where(src == iota((capacity, sources), 1), 1.0, 0.0).astype(bf16)
    extra = recv_ref[:, blocks * most : blocks * most + EXTRA, :].astype(f32)
    lanes = iota(wide, 1)
    probs = jnp.zeros((capacity, 1), f32)
    for k in range(2):
        table = jnp.zeros(wide, f32)
        for part in range(3):
            table = table + mm(pick, extra[:, 2 * part + k, :].astype(bf16))
        probs = probs + jnp.sum(
            jnp.where(lanes + k * LANES == local, table, 0.0), axis=1, keepdims=True
        )
    probs_ref[...] = jnp.broadcast_to(probs, wide)


def hidden_kernel(here_ref, *refs, offsets):
    chunks = refs[: len(offsets)]
    win_ref, wout_ref, out_ref = refs[len(offsets) :]
    devices = out_ref.shape[0]
    capacity, both = chunks[0].shape
    cols = both // 2
    pre = back = None
    for chunk, offset in zip(chunks, offsets):
        block = lax.rem(here_ref[0] + offset + devices, devices)
        span = pl.ds(pl.multiple_of(block * cols, cols), cols)
        one = mm(chunk[:, :cols], win_ref[span, :])
        two = mm(chunk[:, cols:], wout_ref[:, span], ((1,), (1,)))
        pre = one if pre is None else pre + one
        back = two if back is None else back + two
    cumulative = 0.5 * (1.0 + lax.erf(pre * inv_root_two))
    slopes = cumulative + pre * jnp.exp(-0.5 * pre * pre) * inv_root_tau
    gates = jnp.sum(pre * cumulative * back, axis=1, keepdims=True)
    delta = (back * slopes).astype(bf16)
    for d in range(devices):
        block = mm(delta, win_ref[d * cols : (d + 1) * cols, :], ((1,), (1,))).astype(bf16)
        for k in range(cols // LANES):
            out_ref[d, k * capacity : (k + 1) * capacity, :] = block[:, k * LANES : (k + 1) * LANES]
    gates = column_to_row(gates)
    rows = []
    for part in in_parts(gates, 3):
        rows += [part[:, k : k + LANES] for k in range(0, capacity, LANES)]
    extra = stacked_rows(rows, EXTRA).astype(bf16)
    at = cols // LANES * capacity
    out_ref[:, at : at + EXTRA, :] = jnp.broadcast_to(extra, (devices, EXTRA, LANES))


def combine_kernel(here_ref, parts_ref, probs_ref, own_ref, router_ref, place_ref, out_ref):
    devices = parts_ref.shape[0]
    capacity, both = own_ref.shape
    cols = both // 2
    blocks = cols // LANES
    sources = out_ref.shape[0]
    most = place_ref.shape[0] // sources
    at = blocks * capacity
    extra = jnp.sum(parts_ref[:, at : at + EXTRA, :].astype(f32), axis=0)
    per = capacity // LANES
    gates = extra[:per] + extra[per : 2 * per] + extra[2 * per : 3 * per]
    gates = jnp.concatenate([row_to_column(gates[k : k + 1]) for k in range(per)], axis=0)
    probs = probs_ref[...]
    logit_grad = (probs * (1.0 - probs) * gates).astype(bf16).astype(f32)
    router = router_ref[...].astype(f32)
    mine = iota(router.shape, 0) == here_ref[0]
    router = jnp.sum(jnp.where(mine, router, 0.0), axis=0, keepdims=True)
    rows, own = [[], []], own_ref[:, :cols].astype(f32)
    for k in range(blocks):
        total = jnp.zeros((capacity, LANES), f32)
        for d in range(devices):
            total = total + parts_ref[d, k * capacity : (k + 1) * capacity, :].astype(f32)
        cut = slice(k * LANES, (k + 1) * LANES)
        block = (total * probs + logit_grad * router[:, cut]).astype(bf16)
        block = mm(place_ref[...], block).astype(bf16).reshape(sources, most, LANES)
        out_ref[:, k * most : (k + 1) * most, :] = block
        column = jnp.sum(own[:, cut] * logit_grad, axis=0, keepdims=True)
        for into, part in zip(rows, in_parts(column, 2)):
            into.append(part)
    extra = stacked_rows(rows[0] + rows[1], EXTRA).astype(bf16)
    out_ref[:, blocks * most : blocks * most + EXTRA, :] = jnp.broadcast_to(
        extra, (sources, EXTRA, LANES)
    )


def finish_kernel(recv_ref, pick_ref, grad_ref, router_ref):
    experts = recv_ref.shape[0]
    most = pick_ref.shape[0] // experts
    blocks = grad_ref.shape[1] // LANES
    extra = recv_ref[:, blocks * most : blocks * most + EXTRA, :].astype(f32)
    rows = []
    for k in range(blocks):
        rows.append(recv_ref[:, k * most : (k + 1) * most, :].reshape(experts * most, LANES))
        router_ref[:, k * LANES : (k + 1) * LANES] = extra[:, k, :] + extra[:, blocks + k, :]
    grad_ref[...] = mm(pick_ref[...], jnp.concatenate(rows, axis=1), ((0,), (0,)))


def kernel_call(body, outs, scalars, *args):
    vmem = pl.BlockSpec(memory_space=pltpu.VMEM)
    smem = pl.BlockSpec(memory_space=pltpu.SMEM)
    shapes = [jax.ShapeDtypeStruct(s, t) for s, t in outs]
    return pl.pallas_call(
        body,
        out_shape=shapes,
        in_specs=[smem] * scalars + [vmem] * (len(args) - scalars),
        out_specs=[vmem] * len(shapes),
    )(*args)


def ring_gather(x, axis):
    n = lax.axis_size(axis)
    up = [(k, (k + 1) % n) for k in range(n)]
    down = [(k, (k - 1) % n) for k in range(n)]
    chunks, offsets = [x], [0]
    right = left = x
    for step in range(1, n // 2 + 1):
        right = lax.ppermute(right, axis, up)
        chunks.append(right)
        offsets.append(-step)
        if 2 * step < n:
            left = lax.ppermute(left, axis, down)
            chunks.append(left)
            offsets.append(step)
    return chunks, tuple(offsets)


def per_device(tokens_in, out_grad, logits, indices, w_in, w_out, router_w):
    tok, cols = tokens_in.shape
    experts, capacity = indices.shape
    most = min(tok, 2 * capacity // experts)
    spread = experts * most
    devices = lax.axis_size("mp")
    here = lax.axis_index("expert")
    own = lax.dynamic_slice_in_dim(indices, here, 1, 0)
    here = here.reshape(1)
    there = lax.axis_index("mp").reshape(1)
    blocks = cols // LANES
    send, pick = kernel_call(
        pack_kernel,
        [((experts, 2 * blocks * most + EXTRA, LANES), bf16), ((spread, tok), bf16)],
        1,
        here,
        indices,
        tokens_in,
        out_grad,
        logits.T,
    )
    recv = lax.all_to_all(send, "expert", 0, 0, tiled=True)
    rows, probs, place = kernel_call(
        compact_kernel,
        [((capacity, 2 * cols), bf16), ((capacity, LANES), f32), ((spread, capacity), bf16)],
        0,
        own,
        recv,
    )
    chunks, offsets = ring_gather(rows, "mp")
    (parts,) = kernel_call(
        functools.partial(hidden_kernel, offsets=offsets),
        [((devices, blocks * capacity + EXTRA, LANES), bf16)],
        1,
        there,
        *chunks,
        w_in[0],
        w_out[0],
    )
    parts = lax.all_to_all(parts, "mp", 0, 0, tiled=True)
    (back,) = kernel_call(
        combine_kernel,
        [((experts, blocks * most + EXTRA, LANES), bf16)],
        1,
        here,
        parts,
        probs,
        rows,
        router_w.T,
        place,
    )
    back = lax.all_to_all(back, "expert", 0, 0, tiled=True)
    input_grad, router_grad = kernel_call(
        finish_kernel, [((tok, cols), f32), ((experts, cols), f32)], 0, back, pick
    )
    return input_grad, router_grad.T


def solution(mesh):
    return jax.shard_map(
        per_device,
        mesh=mesh,
        in_specs=(
            P(("groups", "expert"), "mp"),
            P(("groups", "expert"), "mp"),
            P(("groups", "expert"), None),
            P("groups", None),
            P("expert", None, "mp"),
            P("expert", "mp", None),
            P("mp", None),
        ),
        out_specs=(P(("groups", "expert"), "mp"), P(("groups", "mp"), None)),
        check_vma=False,
    )
```

```python
import functools

import jax
import jax.numpy as jnp
from jax import lax
from jax.experimental import pallas as pl
from jax.experimental.pallas import tpu as pltpu
from jax.sharding import PartitionSpec as P


inv_root_two = 0.7071067811865476
inv_root_tau = 0.3989422804014327
LANES = 128
EXTRA = 8
SCOPED = 16 * 2**20
f32 = jnp.float32
bf16 = jnp.bfloat16
i32 = jnp.int32


def mm(a, b, contract=((1,), (0,))):
    return lax.dot_general(a, b, (contract, ((), ())), preferred_element_type=f32)


def iota(shape, dim):
    return lax.broadcasted_iota(i32, shape, dim)


def in_parts(v, parts):
    out = []
    for _ in range(parts):
        part = v.astype(bf16).astype(f32)
        out.append(part)
        v = v - part
    return out


def row_to_column(row):
    n = row.shape[1]
    eye = iota((n, n), 0) == iota((n, n), 1)
    return jnp.sum(jnp.where(eye, row, jnp.zeros_like(row)), axis=1, keepdims=True)


def column_to_row(column):
    n = column.shape[0]
    eye = iota((n, n), 0) == iota((n, n), 1)
    return jnp.sum(jnp.where(eye, column, jnp.zeros_like(column)), axis=0, keepdims=True)


def stacked_rows(rows, height):
    count = rows[0].shape[0]
    at = iota((count, height, LANES), 1)
    out = jnp.zeros((count, height, LANES), f32)
    for k, row in enumerate(rows):
        out = jnp.where(at == k, row[:, None, :], out)
    return out


def pack_kernel(here_ref, idx_ref, tok_ref, grad_ref, logit_ref, send_ref, pick_ref):
    experts, capacity = idx_ref.shape
    tok, cols = tok_ref.shape
    most = pick_ref.shape[0] // experts
    local = idx_ref[...] - here_ref[0] * tok
    token = iota((experts, tok), 1)
    member = jnp.zeros((experts, tok), i32)
    for c in range(capacity):
        member = jnp.where(local[:, c : c + 1] == token, 1, member)
    before = (iota((tok, tok), 0) < iota((tok, tok), 1)).astype(f32).astype(bf16)
    rank = mm(member.astype(f32).astype(bf16), before).astype(i32)
    rank = jnp.where(member == 1, rank, -1)
    ranks = iota((most, tok), 0)
    for e in range(experts):
        hit = jnp.where(rank[e : e + 1, :] == ranks, 1.0, 0.0)
        pick_ref[e * most : (e + 1) * most, :] = hit.astype(bf16)
    pick = pick_ref[...]
    at = 0
    for ref in (tok_ref, grad_ref):
        rows = mm(pick, ref[...]).astype(bf16)
        for k in range(0, cols, LANES):
            send_ref[:, at : at + most, :] = rows[:, k : k + LANES].reshape(experts, most, LANES)
            at += most
    probs = jax.nn.sigmoid(logit_ref[...])
    rows = []
    for part in in_parts(probs, 3):
        rows += [part[:, k : k + LANES] for k in range(0, tok, LANES)]
    send_ref[:, at : at + EXTRA, :] = stacked_rows(rows, EXTRA).astype(bf16)


def compact_kernel(here_ref, idx_ref, recv_ref, rows_ref, probs_ref, place_ref):
    sources = recv_ref.shape[0]
    capacity = idx_ref.shape[1]
    spread = place_ref.shape[0]
    most = spread // sources
    tok = 2 * LANES
    square = (capacity, capacity)
    own_row = idx_ref[pl.ds(here_ref[0], 1), :]
    own_col = row_to_column(own_row)
    pos_row = jnp.sum((own_col < own_row).astype(i32), axis=0, keepdims=True)
    token = jnp.sum(jnp.where(pos_row == iota(square, 0), own_row, 0), axis=1, keepdims=True)
    src = token // tok
    local = token - src * tok
    wide = (capacity, LANES)
    start = jnp.sum((own_col < iota(wide, 1) * tok).astype(i32), axis=0, keepdims=True)
    is_src = src == iota(wide, 1)
    first = jnp.sum(jnp.where(is_src, start, 0), axis=1, keepdims=True)
    target = src * most + iota((capacity, 1), 0) - first
    place = jnp.where(target == iota((capacity, spread), 1), 1.0, 0.0).astype(bf16)
    place_ref[...] = jnp.where(
        column_to_row(target) == iota((spread, capacity), 0), 1.0, 0.0
    ).astype(bf16)
    blocks = rows_ref.shape[1] // LANES
    for k in range(blocks):
        block = recv_ref[:, k * most : (k + 1) * most, :].reshape(spread, LANES)
        rows_ref[:, k * LANES : (k + 1) * LANES] = mm(place, block).astype(bf16)
    pick = jnp.where(src == iota((capacity, sources), 1), 1.0, 0.0).astype(bf16)
    extra = recv_ref[:, blocks * most : blocks * most + EXTRA, :].astype(f32)
    lanes = iota(wide, 1)
    probs = jnp.zeros((capacity, 1), f32)
    for k in range(2):
        table = jnp.zeros(wide, f32)
        for part in range(3):
            table = table + mm(pick, extra[:, 2 * part + k, :].astype(bf16))
        probs = probs + jnp.sum(
            jnp.where(lanes + k * LANES == local, table, 0.0), axis=1, keepdims=True
        )
    probs_ref[...] = jnp.broadcast_to(probs, wide)


def products(here_ref, chunks, offsets, win_ref, wout_ref, devices, pre=None, back=None):
    cols = win_ref.shape[0] // devices
    for chunk, offset in zip(chunks, offsets):
        block = lax.rem(here_ref[1] + offset + devices, devices)
        span = pl.ds(pl.multiple_of(block * cols, cols), cols)
        one = mm(chunk[:, :cols], win_ref[span, :])
        two = mm(chunk[:, cols:], wout_ref[:, span], ((1,), (1,)))
        pre = one if pre is None else pre + one
        back = two if back is None else back + two
    return pre, back


def first_kernel(here_ref, *refs, offsets, devices):
    chunks = refs[: len(offsets)]
    win_ref, wout_ref, pre_ref, back_ref = refs[len(offsets) :]
    pre_ref[...], back_ref[...] = products(
        here_ref, chunks, offsets, win_ref, wout_ref, devices
    )


def hidden_kernel(here_ref, pre_ref, back_ref, *refs, offsets):
    chunks = refs[: len(offsets)]
    win_ref, wout_ref, out_ref = refs[len(offsets) :]
    devices = out_ref.shape[0]
    capacity, both = chunks[0].shape
    cols = both // 2
    pre, back = products(
        here_ref, chunks, offsets, win_ref, wout_ref, devices, pre_ref[...], back_ref[...]
    )
    cumulative = 0.5 * (1.0 + lax.erf(pre * inv_root_two))
    slopes = cumulative + pre * jnp.exp(-0.5 * pre * pre) * inv_root_tau
    gates = jnp.sum(pre * cumulative * back, axis=1, keepdims=True)
    delta = (back * slopes).astype(bf16)
    for d in range(devices):
        block = mm(delta, win_ref[d * cols : (d + 1) * cols, :], ((1,), (1,))).astype(bf16)
        for k in range(cols // LANES):
            out_ref[d, k * capacity : (k + 1) * capacity, :] = block[:, k * LANES : (k + 1) * LANES]
    gates = column_to_row(gates)
    rows = []
    for part in in_parts(gates, 3):
        rows += [part[:, k : k + LANES] for k in range(0, capacity, LANES)]
    extra = stacked_rows(rows, EXTRA).astype(bf16)
    at = cols // LANES * capacity
    out_ref[:, at : at + EXTRA, :] = jnp.broadcast_to(extra, (devices, EXTRA, LANES))


def combine_kernel(here_ref, parts_ref, probs_ref, own_ref, router_ref, place_ref, out_ref):
    devices = parts_ref.shape[0]
    capacity, both = own_ref.shape
    cols = both // 2
    blocks = cols // LANES
    sources = out_ref.shape[0]
    most = place_ref.shape[0] // sources
    at = blocks * capacity
    extra = jnp.sum(parts_ref[:, at : at + EXTRA, :].astype(f32), axis=0)
    per = capacity // LANES
    gates = extra[:per] + extra[per : 2 * per] + extra[2 * per : 3 * per]
    gates = jnp.concatenate([row_to_column(gates[k : k + 1]) for k in range(per)], axis=0)
    probs = probs_ref[...]
    logit_grad = (probs * (1.0 - probs) * gates).astype(bf16).astype(f32)
    router = router_ref[...].astype(f32)
    mine = iota(router.shape, 0) == here_ref[0]
    router = jnp.sum(jnp.where(mine, router, 0.0), axis=0, keepdims=True)
    rows, own = [[], []], own_ref[:, :cols].astype(f32)
    for k in range(blocks):
        total = jnp.zeros((capacity, LANES), f32)
        for d in range(devices):
            total = total + parts_ref[d, k * capacity : (k + 1) * capacity, :].astype(f32)
        cut = slice(k * LANES, (k + 1) * LANES)
        block = (total * probs + logit_grad * router[:, cut]).astype(bf16)
        block = mm(place_ref[...], block).astype(bf16).reshape(sources, most, LANES)
        out_ref[:, k * most : (k + 1) * most, :] = block
        column = jnp.sum(own[:, cut] * logit_grad, axis=0, keepdims=True)
        for into, part in zip(rows, in_parts(column, 2)):
            into.append(part)
    extra = stacked_rows(rows[0] + rows[1], EXTRA).astype(bf16)
    out_ref[:, blocks * most : blocks * most + EXTRA, :] = jnp.broadcast_to(
        extra, (sources, EXTRA, LANES)
    )


def finish_kernel(recv_ref, pick_ref, grad_ref, router_ref):
    experts = recv_ref.shape[0]
    most = pick_ref.shape[0] // experts
    blocks = grad_ref.shape[1] // LANES
    extra = recv_ref[:, blocks * most : blocks * most + EXTRA, :].astype(f32)
    rows = []
    for k in range(blocks):
        rows.append(recv_ref[:, k * most : (k + 1) * most, :].reshape(experts * most, LANES))
        router_ref[:, k * LANES : (k + 1) * LANES] = extra[:, k, :] + extra[:, blocks + k, :]
    grad_ref[...] = mm(pick_ref[...], jnp.concatenate(rows, axis=1), ((0,), (0,)))


def kernel_call(body, outs, scalars, *args, flops=0):
    vmem = pl.BlockSpec(memory_space=pltpu.VMEM)
    smem = pl.BlockSpec(memory_space=pltpu.SMEM)
    shapes = [jax.ShapeDtypeStruct(s, t) for s, t in outs]
    return pl.pallas_call(
        body,
        out_shape=shapes,
        in_specs=[smem] * scalars + [vmem] * (len(args) - scalars),
        out_specs=[vmem] * len(shapes),
        cost_estimate=pl.CostEstimate(flops=flops, transcendentals=0, bytes_accessed=0) if flops else None,
        compiler_params=pltpu.CompilerParams(vmem_limit_bytes=SCOPED),
    )(*args)


def ring_gather(x, axis):
    n = lax.axis_size(axis)
    up = [(k, (k + 1) % n) for k in range(n)]
    down = [(k, (k - 1) % n) for k in range(n)]
    chunks, offsets = [x], [0]
    right = left = x
    for step in range(1, n // 2 + 1):
        right = lax.ppermute(right, axis, up)
        chunks.append(right)
        offsets.append(-step)
        if 2 * step < n:
            left = lax.ppermute(left, axis, down)
            chunks.append(left)
            offsets.append(step)
    return chunks, tuple(offsets)


def per_device(tokens_in, out_grad, logits, indices, w_in, w_out, router_w):
    tok, cols = tokens_in.shape
    experts, capacity = indices.shape
    most = min(tok, 2 * capacity // experts)
    spread = experts * most
    devices = lax.axis_size("mp")
    here = jnp.stack([lax.axis_index("expert"), lax.axis_index("mp")]).astype(i32)
    blocks = cols // LANES
    send, pick = kernel_call(
        pack_kernel,
        [((experts, 2 * blocks * most + EXTRA, LANES), bf16), ((spread, tok), bf16)],
        1,
        here,
        indices,
        tokens_in,
        out_grad,
        logits.T,
    )
    recv = lax.all_to_all(send, "expert", 0, 0, tiled=True)
    rows, probs, place = kernel_call(
        compact_kernel,
        [((capacity, 2 * cols), bf16), ((capacity, LANES), f32), ((spread, capacity), bf16)],
        1,
        here,
        indices,
        recv,
    )
    chunks, offsets = ring_gather(rows, "mp")
    hidden = w_in.shape[2]
    early = len(chunks) - 1
    pre, back = kernel_call(
        functools.partial(first_kernel, offsets=offsets[:early], devices=devices),
        [((capacity, hidden), f32)] * 2,
        1,
        here,
        *chunks[:early],
        w_in[0],
        w_out[0],
        flops=4 * early * capacity * cols * hidden,
    )
    (parts,) = kernel_call(
        functools.partial(hidden_kernel, offsets=offsets[early:]),
        [((devices, blocks * capacity + EXTRA, LANES), bf16)],
        1,
        here,
        pre,
        back,
        *chunks[early:],
        w_in[0],
        w_out[0],
    )
    parts = lax.all_to_all(parts, "mp", 0, 0, tiled=True)
    (back,) = kernel_call(
        combine_kernel,
        [((experts, blocks * most + EXTRA, LANES), bf16)],
        1,
        here,
        parts,
        probs,
        rows,
        router_w.T,
        place,
    )
    back = lax.all_to_all(back, "expert", 0, 0, tiled=True)
    input_grad, router_grad = kernel_call(
        finish_kernel, [((tok, cols), f32), ((experts, cols), f32)], 0, back, pick
    )
    return input_grad, router_grad.T


def solution(mesh):
    return jax.shard_map(
        per_device,
        mesh=mesh,
        in_specs=(
            P(("groups", "expert"), "mp"),
            P(("groups", "expert"), "mp"),
            P(("groups", "expert"), None),
            P("groups", None),
            P("expert", None, "mp"),
            P("expert", "mp", None),
            P("mp", None),
        ),
        out_specs=(P(("groups", "expert"), "mp"), P(("groups", "mp"), None)),
        check_vma=False,
    )
```

```python
import functools

import jax
import jax.numpy as jnp
from jax import lax
from jax.experimental import pallas as pl
from jax.experimental.pallas import tpu as pltpu
from jax.sharding import PartitionSpec as P


inv_root_two = 0.7071067811865476
inv_root_tau = 0.3989422804014327
LANES = 128
EXTRA = 8
SENT = 4
BACK = 2
SCOPED = 16 * 2**20
f32 = jnp.float32
bf16 = jnp.bfloat16
i32 = jnp.int32


def mm(a, b, contract=((1,), (0,))):
    return lax.dot_general(a, b, (contract, ((), ())), preferred_element_type=f32)


def iota(shape, dim):
    return lax.broadcasted_iota(i32, shape, dim)


def in_parts(v, parts):
    out = []
    for _ in range(parts):
        part = v.astype(bf16).astype(f32)
        out.append(part)
        v = v - part
    return out


def row_to_column(row):
    n = row.shape[1]
    eye = iota((n, n), 0) == iota((n, n), 1)
    return jnp.sum(jnp.where(eye, row, jnp.zeros_like(row)), axis=1, keepdims=True)


def column_to_row(column):
    n = column.shape[0]
    eye = iota((n, n), 0) == iota((n, n), 1)
    return jnp.sum(jnp.where(eye, column, jnp.zeros_like(column)), axis=0, keepdims=True)


def stacked_rows(rows, height):
    count = rows[0].shape[0]
    at = iota((count, height, LANES), 1)
    out = jnp.zeros((count, height, LANES), f32)
    for k, row in enumerate(rows):
        out = jnp.where(at == k, row[:, None, :], out)
    return out


def pack_kernel(here_ref, *refs):
    given, (send_ref, pick_ref, own_ref), held, done = refs[:4], refs[4:7], refs[7:11], refs[11]
    copies = [pltpu.make_async_copy(a, b, done.at[k]) for k, (a, b) in enumerate(zip(given, held))]
    for copy in copies:
        copy.start()
    idx_ref, tok_ref, grad_ref, logit_ref = held
    copies[0].wait()
    own_ref[...] = idx_ref[pl.ds(here_ref[0], 1), :]
    experts, capacity = idx_ref.shape
    tok, cols = tok_ref.shape
    most = pick_ref.shape[0] // experts
    local = idx_ref[...] - here_ref[0] * tok
    token = iota((experts, tok), 1)
    member = jnp.zeros((experts, tok), i32)
    for c in range(capacity):
        member = jnp.where(local[:, c : c + 1] == token, 1, member)
    before = (iota((tok, tok), 0) < iota((tok, tok), 1)).astype(f32).astype(bf16)
    rank = mm(member.astype(f32).astype(bf16), before).astype(i32)
    rank = jnp.where(member == 1, rank, -1)
    ranks = iota((most, tok), 0)
    for e in range(experts):
        hit = jnp.where(rank[e : e + 1, :] == ranks, 1.0, 0.0)
        pick_ref[e * most : (e + 1) * most, :] = hit.astype(bf16)
    pick = pick_ref[...]
    height = send_ref.shape[0] // experts
    at = 0
    for ref, copy in ((tok_ref, copies[1]), (grad_ref, copies[2])):
        copy.wait()
        rows = mm(pick, ref[...]).astype(bf16)
        for k in range(0, cols, LANES):
            for e in range(experts):
                to = e * height + at
                send_ref[to : to + most, :] = rows[e * most : (e + 1) * most, k : k + LANES]
            at += most
    copies[3].wait()
    rows = []
    for part in in_parts(logit_ref[...], 2):
        rows += [part[:, k : k + LANES] for k in range(0, tok, LANES)]
    extra = stacked_rows(rows, EXTRA).astype(bf16)
    for e in range(experts):
        to = e * height + at
        send_ref[to : to + SENT, :] = extra[e, :SENT]


def compact_kernel(own_ref, recv_ref, rows_ref, probs_ref, back_ref, got_ref, extra_ref, *, tok):
    spread, capacity = back_ref.shape
    sources = extra_ref.shape[1]
    most = spread // sources
    square = (capacity, capacity)
    own_row = own_ref[...]
    own_col = row_to_column(own_row)
    pos_row = jnp.sum((own_col < own_row).astype(i32), axis=0, keepdims=True)
    token = jnp.sum(jnp.where(pos_row == iota(square, 0), own_row, 0), axis=1, keepdims=True)
    src = token // tok
    local = token - src * tok
    wide = (capacity, LANES)
    start = jnp.sum((own_col < iota(wide, 1) * tok).astype(i32), axis=0, keepdims=True)
    first = jnp.sum(jnp.where(src == iota(wide, 1), start, 0), axis=1, keepdims=True)
    target = src * most + iota((capacity, 1), 0) - first
    place = jnp.where(target == iota((capacity, spread), 1), 1.0, 0.0).astype(bf16)
    back = jnp.where(column_to_row(target) == iota((spread, capacity), 0), 1.0, 0.0)
    back_ref[...] = back.astype(bf16)
    pick = jnp.where(src == iota((capacity, sources), 1), 1.0, 0.0).astype(bf16)
    height = recv_ref.shape[0] // sources
    blocks = rows_ref.shape[1] // LANES
    for e in range(sources):
        for k in range(blocks):
            at = e * height + k * most
            got_ref[e * most : (e + 1) * most, k * LANES : (k + 1) * LANES] = recv_ref[
                at : at + most, :
            ]
        extra = recv_ref[e * height + blocks * most : (e + 1) * height, :].astype(f32)
        for k in range(SENT):
            extra_ref[k, e : e + 1, :] = extra[k : k + 1]
    rows_ref[...] = mm(place, got_ref[...]).astype(bf16)
    lanes = iota(wide, 1)
    per = SENT // 2
    logits = jnp.zeros((capacity, 1), f32)
    for k in range(per):
        table = mm(pick, extra_ref[k].astype(bf16)) + mm(pick, extra_ref[per + k].astype(bf16))
        hit = lanes + k * LANES == local
        logits = logits + jnp.sum(jnp.where(hit, table, 0.0), axis=1, keepdims=True)
    probs_ref[...] = jax.nn.sigmoid(jnp.broadcast_to(logits, (capacity, LANES)))


def products(here_ref, chunks, offsets, win_ref, wout_ref, devices, pre=None, back=None):
    cols = win_ref.shape[0] // devices
    for chunk, offset in zip(chunks, offsets):
        block = lax.rem(here_ref[1] + offset + devices, devices)
        span = pl.ds(pl.multiple_of(block * cols, cols), cols)
        one = mm(chunk[:, :cols], win_ref[span, :])
        two = mm(chunk[:, cols:], wout_ref[:, span], ((1,), (1,)))
        pre = one if pre is None else pre + one
        back = two if back is None else back + two
    return pre, back


def first_kernel(here_ref, *refs, offsets, devices):
    chunks = refs[: len(offsets)]
    win_ref, wout_ref, pre_ref, back_ref = refs[len(offsets) :]
    pre_ref[...], back_ref[...] = products(
        here_ref, chunks, offsets, win_ref, wout_ref, devices
    )


def hidden_kernel(here_ref, pre_ref, back_ref, *refs, offsets):
    chunks = refs[: len(offsets)]
    win_ref, wout_ref, out_ref = refs[len(offsets) :]
    devices = out_ref.shape[0]
    capacity, both = chunks[0].shape
    cols = both // 2
    pre, back = products(
        here_ref, chunks, offsets, win_ref, wout_ref, devices, pre_ref[...], back_ref[...]
    )
    cumulative = 0.5 * (1.0 + lax.erf(pre * inv_root_two))
    slopes = cumulative + pre * jnp.exp(-0.5 * pre * pre) * inv_root_tau
    gates = jnp.sum(pre * cumulative * back, axis=1, keepdims=True)
    delta = (back * slopes).astype(bf16)
    for d in range(devices):
        block = mm(delta, win_ref[d * cols : (d + 1) * cols, :], ((1,), (1,))).astype(bf16)
        for k in range(cols // LANES):
            out_ref[d, k * capacity : (k + 1) * capacity, :] = block[:, k * LANES : (k + 1) * LANES]
    gates = column_to_row(gates)
    rows = []
    for part in in_parts(gates, 3):
        rows += [part[:, k : k + LANES] for k in range(0, capacity, LANES)]
    extra = stacked_rows(rows, EXTRA).astype(bf16)
    at = cols // LANES * capacity
    out_ref[:, at : at + EXTRA, :] = jnp.broadcast_to(extra, (devices, EXTRA, LANES))


def combine_kernel(here_ref, parts_ref, probs_ref, own_ref, router_ref, place_ref, out_ref):
    devices = parts_ref.shape[0]
    capacity, both = own_ref.shape
    cols = both // 2
    blocks = cols // LANES
    sources = router_ref.shape[0]
    most = place_ref.shape[0] // sources
    height = out_ref.shape[0] // sources
    at = blocks * capacity
    extra = jnp.sum(parts_ref[:, at : at + EXTRA, :].astype(f32), axis=0)
    per = capacity // LANES
    gates = extra[:per] + extra[per : 2 * per] + extra[2 * per : 3 * per]
    gates = jnp.concatenate([row_to_column(gates[k : k + 1]) for k in range(per)], axis=0)
    probs = probs_ref[...]
    logit_grad = (probs * (1.0 - probs) * gates).astype(bf16).astype(f32)
    router = router_ref[...].astype(f32)
    mine = iota(router.shape, 0) == here_ref[0]
    router = jnp.sum(jnp.where(mine, router, 0.0), axis=0, keepdims=True)
    rows, own = [], own_ref[:, :cols].astype(f32)
    for k in range(blocks):
        total = jnp.zeros((capacity, LANES), f32)
        for d in range(devices):
            total = total + parts_ref[d, k * capacity : (k + 1) * capacity, :].astype(f32)
        cut = slice(k * LANES, (k + 1) * LANES)
        block = (total * probs + logit_grad * router[:, cut]).astype(bf16)
        block = mm(place_ref[...], block).astype(bf16)
        for e in range(sources):
            to = e * height + k * most
            out_ref[to : to + most, :] = block[e * most : (e + 1) * most]
        rows.append(jnp.sum(own[:, cut] * logit_grad, axis=0, keepdims=True))
    extra = stacked_rows(rows, EXTRA).astype(bf16)
    for e in range(sources):
        out_ref[(e + 1) * height - BACK : (e + 1) * height, :] = extra[0, :BACK]


def finish_kernel(recv_ref, pick_ref, grad_ref, router_ref, got_ref):
    experts = router_ref.shape[0]
    most = pick_ref.shape[0] // experts
    height = recv_ref.shape[0] // experts
    blocks = grad_ref.shape[1] // LANES
    for e in range(experts):
        extra = recv_ref[(e + 1) * height - BACK : (e + 1) * height, :].astype(f32)
        for k in range(blocks):
            cut = slice(k * LANES, (k + 1) * LANES)
            at = e * height + k * most
            got_ref[e * most : (e + 1) * most, cut] = recv_ref[at : at + most, :]
            router_ref[e : e + 1, cut] = extra[k : k + 1]
    grad_ref[...] = mm(pick_ref[...], got_ref[...], ((0,), (0,)))


def exchanged(x, axis):
    shape = (lax.axis_size(axis), -1, 2, LANES)
    return lax.all_to_all(x.reshape(shape), axis, 0, 0, tiled=True).reshape(x.shape)


def kernel_call(body, outs, scalars, *args, flops=0, space=pltpu.VMEM, scratch=()):
    vmem = pl.BlockSpec(memory_space=pltpu.VMEM)
    smem = pl.BlockSpec(memory_space=pltpu.SMEM)
    held = pl.BlockSpec(memory_space=space)
    shapes = [jax.ShapeDtypeStruct(s, t) for s, t in outs]
    return pl.pallas_call(
        body,
        out_shape=shapes,
        in_specs=[smem] * scalars + [held] * (len(args) - scalars),
        out_specs=[vmem] * len(shapes),
        scratch_shapes=list(scratch),
        cost_estimate=pl.CostEstimate(flops=flops, transcendentals=0, bytes_accessed=0) if flops else None,
        compiler_params=pltpu.CompilerParams(vmem_limit_bytes=SCOPED),
    )(*args)


def ring_gather(x, axis):
    n = lax.axis_size(axis)
    up = [(k, (k + 1) % n) for k in range(n)]
    down = [(k, (k - 1) % n) for k in range(n)]
    chunks, offsets = [x], [0]
    right = left = x
    for step in range(1, n // 2 + 1):
        left = lax.ppermute(left, axis, down)
        chunks.append(left)
        offsets.append(step)
        if 2 * step < n:
            right = lax.ppermute(right, axis, up)
            chunks.append(right)
            offsets.append(-step)
    return chunks, tuple(offsets)


def per_device(tokens_in, out_grad, logits, indices, w_in, w_out, router_w):
    tok, cols = tokens_in.shape
    experts, capacity = indices.shape
    most = min(tok, 2 * capacity // experts)
    spread = experts * most
    devices = lax.axis_size("mp")
    here = jnp.stack([lax.axis_index("expert"), lax.axis_index("mp")]).astype(i32)
    blocks = cols // LANES
    given = (indices, tokens_in, out_grad, logits.T)
    send, pick, own = kernel_call(
        pack_kernel,
        [
            ((experts * (2 * blocks * most + SENT), LANES), bf16),
            ((spread, tok), bf16),
            ((1, capacity), i32),
        ],
        1,
        here,
        *(pltpu.with_memory_space_constraint(x, pltpu.HBM) for x in given),
        space=pltpu.HBM,
        scratch=[pltpu.VMEM(x.shape, x.dtype) for x in given] + [pltpu.SemaphoreType.DMA((4,))],
    )
    recv = exchanged(send, "expert")
    rows, probs, place_back = kernel_call(
        functools.partial(compact_kernel, tok=tok),
        [((capacity, 2 * cols), bf16), ((capacity, LANES), f32), ((spread, capacity), bf16)],
        0,
        own,
        recv,
        scratch=[pltpu.VMEM((spread, 2 * cols), bf16), pltpu.VMEM((SENT, experts, LANES), f32)],
    )
    chunks, offsets = ring_gather(rows, "mp")
    hidden = w_in.shape[2]
    early = len(chunks) - 1
    pre, back = kernel_call(
        functools.partial(first_kernel, offsets=offsets[:early], devices=devices),
        [((capacity, hidden), f32)] * 2,
        1,
        here,
        *chunks[:early],
        w_in[0],
        w_out[0],
        flops=4 * early * capacity * cols * hidden,
    )
    (parts,) = kernel_call(
        functools.partial(hidden_kernel, offsets=offsets[early:]),
        [((devices, blocks * capacity + EXTRA, LANES), bf16)],
        1,
        here,
        pre,
        back,
        *chunks[early:],
        w_in[0],
        w_out[0],
    )
    parts = lax.all_to_all(parts, "mp", 0, 0, tiled=True)
    (back,) = kernel_call(
        combine_kernel,
        [((experts * (blocks * most + BACK), LANES), bf16)],
        1,
        here,
        parts,
        probs,
        rows,
        router_w.T,
        place_back,
    )
    back = exchanged(back, "expert")
    input_grad, router_grad = kernel_call(
        finish_kernel,
        [((tok, cols), f32), ((experts, cols), f32)],
        0,
        back,
        pick,
        scratch=[pltpu.VMEM((spread, cols), bf16)],
    )
    return input_grad, router_grad.T


def solution(mesh):
    return jax.shard_map(
        per_device,
        mesh=mesh,
        in_specs=(
            P(("groups", "expert"), "mp"),
            P(("groups", "expert"), "mp"),
            P(("groups", "expert"), None),
            P("groups", None),
            P("expert", None, "mp"),
            P("expert", "mp", None),
            P("mp", None),
        ),
        out_specs=(P(("groups", "expert"), "mp"), P(("groups", "mp"), None)),
        check_vma=False,
    )
```

```python
import functools

import jax
import jax.numpy as jnp
from jax import lax
from jax.experimental import pallas as pl
from jax.experimental.pallas import tpu as pltpu
from jax.sharding import PartitionSpec as P


inv_root_two = 0.7071067811865476
inv_root_tau = 0.3989422804014327
LANES = 128
EXTRA = 8
SENT = 4
BACK = 2
SCOPED = 16 * 2**20
f32 = jnp.float32
bf16 = jnp.bfloat16
i32 = jnp.int32


def mm(a, b, contract=((1,), (0,))):
    return lax.dot_general(a, b, (contract, ((), ())), preferred_element_type=f32)


def iota(shape, dim):
    return lax.broadcasted_iota(i32, shape, dim)


def in_parts(v, parts):
    out = []
    for _ in range(parts):
        part = v.astype(bf16).astype(f32)
        out.append(part)
        v = v - part
    return out


def row_to_column(row):
    n = row.shape[1]
    eye = iota((n, n), 0) == iota((n, n), 1)
    return jnp.sum(jnp.where(eye, row, jnp.zeros_like(row)), axis=1, keepdims=True)


def column_to_row(column):
    n = column.shape[0]
    eye = iota((n, n), 0) == iota((n, n), 1)
    return jnp.sum(jnp.where(eye, column, jnp.zeros_like(column)), axis=0, keepdims=True)


def stacked_rows(rows, height):
    count = rows[0].shape[0]
    at = iota((count, height, LANES), 1)
    out = jnp.zeros((count, height, LANES), f32)
    for k, row in enumerate(rows):
        out = jnp.where(at == k, row[:, None, :], out)
    return out


def pack_kernel(*refs):
    given, (send_ref, pick_ref, own_ref), held, done = refs[:6], refs[6:9], refs[11:15], refs[15]
    held += refs[9:11]
    copies = [pltpu.make_async_copy(a, b, done.at[k]) for k, (a, b) in enumerate(zip(given, held))]
    for copy in copies:
        copy.start()
    idx_ref, tok_ref, grad_ref, logit_ref = held[:4]
    copies[0].wait()
    own_ref[...] = idx_ref[pl.ds(lax.axis_index("expert"), 1), :]
    experts, capacity = idx_ref.shape
    tok, cols = tok_ref.shape
    most = pick_ref.shape[0] // experts
    local = idx_ref[...] - lax.axis_index("expert") * tok
    token = iota((experts, tok), 1)
    member = jnp.zeros((experts, tok), i32)
    for c in range(capacity):
        member = jnp.where(local[:, c : c + 1] == token, 1, member)
    before = (iota((tok, tok), 0) < iota((tok, tok), 1)).astype(f32).astype(bf16)
    rank = mm(member.astype(f32).astype(bf16), before).astype(i32)
    rank = jnp.where(member == 1, rank, -1)
    ranks = iota((most, tok), 0)
    for e in range(experts):
        hit = jnp.where(rank[e : e + 1, :] == ranks, 1.0, 0.0)
        pick_ref[e * most : (e + 1) * most, :] = hit.astype(bf16)
    pick = pick_ref[...]
    height = send_ref.shape[0] // experts
    at = 0
    for ref, copy in ((tok_ref, copies[1]), (grad_ref, copies[2])):
        copy.wait()
        rows = mm(pick, ref[...]).astype(bf16)
        for k in range(0, cols, LANES):
            for e in range(experts):
                to = e * height + at
                send_ref[to : to + most, :] = rows[e * most : (e + 1) * most, k : k + LANES]
            at += most
    copies[3].wait()
    rows = []
    for part in in_parts(logit_ref[...], 2):
        rows += [part[:, k : k + LANES] for k in range(0, tok, LANES)]
    extra = stacked_rows(rows, EXTRA).astype(bf16)
    for e in range(experts):
        to = e * height + at
        send_ref[to : to + SENT, :] = extra[e, :SENT]
    for copy in copies[4:]:
        copy.wait()


def compact_kernel(own_ref, recv_ref, rows_ref, probs_ref, back_ref, got_ref, extra_ref, *, tok):
    spread, capacity = back_ref.shape
    sources = extra_ref.shape[1]
    most = spread // sources
    square = (capacity, capacity)
    own_row = own_ref[...]
    own_col = row_to_column(own_row)
    pos_row = jnp.sum((own_col < own_row).astype(i32), axis=0, keepdims=True)
    token = jnp.sum(jnp.where(pos_row == iota(square, 0), own_row, 0), axis=1, keepdims=True)
    src = token // tok
    local = token - src * tok
    wide = (capacity, LANES)
    start = jnp.sum((own_col < iota(wide, 1) * tok).astype(i32), axis=0, keepdims=True)
    first = jnp.sum(jnp.where(src == iota(wide, 1), start, 0), axis=1, keepdims=True)
    target = src * most + iota((capacity, 1), 0) - first
    place = jnp.where(target == iota((capacity, spread), 1), 1.0, 0.0).astype(bf16)
    back = jnp.where(column_to_row(target) == iota((spread, capacity), 0), 1.0, 0.0)
    back_ref[...] = back.astype(bf16)
    pick = jnp.where(src == iota((capacity, sources), 1), 1.0, 0.0).astype(bf16)
    height = recv_ref.shape[0] // sources
    blocks = rows_ref.shape[1] // LANES
    for e in range(sources):
        for k in range(blocks):
            at = e * height + k * most
            got_ref[e * most : (e + 1) * most, k * LANES : (k + 1) * LANES] = recv_ref[
                at : at + most, :
            ]
        extra = recv_ref[e * height + blocks * most : (e + 1) * height, :].astype(f32)
        for k in range(SENT):
            extra_ref[k, e : e + 1, :] = extra[k : k + 1]
    rows_ref[...] = mm(place, got_ref[...]).astype(bf16)
    lanes = iota(wide, 1)
    per = SENT // 2
    logits = jnp.zeros((capacity, 1), f32)
    for k in range(per):
        table = mm(pick, extra_ref[k].astype(bf16)) + mm(pick, extra_ref[per + k].astype(bf16))
        hit = lanes + k * LANES == local
        logits = logits + jnp.sum(jnp.where(hit, table, 0.0), axis=1, keepdims=True)
    probs_ref[...] = jax.nn.sigmoid(jnp.broadcast_to(logits, (capacity, LANES)))


def products(chunks, offsets, win_ref, wout_ref, devices, pre=None, back=None):
    cols = win_ref.shape[0] // devices
    for chunk, offset in zip(chunks, offsets):
        block = lax.rem(lax.axis_index("mp") + offset + devices, devices)
        span = pl.ds(pl.multiple_of(block * cols, cols), cols)
        one = mm(chunk[:, :cols], win_ref[span, :])
        two = mm(chunk[:, cols:], wout_ref[:, span], ((1,), (1,)))
        pre = one if pre is None else pre + one
        back = two if back is None else back + two
    return pre, back


def first_kernel(*refs, offsets, devices):
    chunks = refs[: len(offsets)]
    win_ref, wout_ref, pre_ref, back_ref = refs[len(offsets) :]
    pre_ref[...], back_ref[...] = products(
        chunks, offsets, win_ref, wout_ref, devices
    )


def hidden_kernel(pre_ref, back_ref, *refs, offsets):
    chunks = refs[: len(offsets)]
    win_ref, wout_ref, out_ref = refs[len(offsets) :]
    devices = out_ref.shape[0]
    capacity, both = chunks[0].shape
    cols = both // 2
    pre, back = products(
        chunks, offsets, win_ref, wout_ref, devices, pre_ref[...], back_ref[...]
    )
    cumulative = 0.5 * (1.0 + lax.erf(pre * inv_root_two))
    slopes = cumulative + pre * jnp.exp(-0.5 * pre * pre) * inv_root_tau
    gates = jnp.sum(pre * cumulative * back, axis=1, keepdims=True)
    delta = (back * slopes).astype(bf16)
    for d in range(devices):
        block = mm(delta, win_ref[d * cols : (d + 1) * cols, :], ((1,), (1,))).astype(bf16)
        for k in range(cols // LANES):
            out_ref[d, k * capacity : (k + 1) * capacity, :] = block[:, k * LANES : (k + 1) * LANES]
    gates = column_to_row(gates)
    rows = []
    for part in in_parts(gates, 3):
        rows += [part[:, k : k + LANES] for k in range(0, capacity, LANES)]
    extra = stacked_rows(rows, EXTRA).astype(bf16)
    at = cols // LANES * capacity
    out_ref[:, at : at + EXTRA, :] = jnp.broadcast_to(extra, (devices, EXTRA, LANES))


def combine_kernel(parts_ref, probs_ref, own_ref, router_ref, place_ref, out_ref):
    devices = parts_ref.shape[0]
    capacity, both = own_ref.shape
    cols = both // 2
    blocks = cols // LANES
    sources = router_ref.shape[0]
    most = place_ref.shape[0] // sources
    height = out_ref.shape[0] // sources
    at = blocks * capacity
    extra = jnp.sum(parts_ref[:, at : at + EXTRA, :].astype(f32), axis=0)
    per = capacity // LANES
    gates = extra[:per] + extra[per : 2 * per] + extra[2 * per : 3 * per]
    gates = jnp.concatenate([row_to_column(gates[k : k + 1]) for k in range(per)], axis=0)
    probs = probs_ref[...]
    logit_grad = (probs * (1.0 - probs) * gates).astype(bf16).astype(f32)
    router = router_ref[...].astype(f32)
    mine = iota(router.shape, 0) == lax.axis_index("expert")
    router = jnp.sum(jnp.where(mine, router, 0.0), axis=0, keepdims=True)
    rows, own = [], own_ref[:, :cols].astype(f32)
    for k in range(blocks):
        total = jnp.zeros((capacity, LANES), f32)
        for d in range(devices):
            total = total + parts_ref[d, k * capacity : (k + 1) * capacity, :].astype(f32)
        cut = slice(k * LANES, (k + 1) * LANES)
        block = (total * probs + logit_grad * router[:, cut]).astype(bf16)
        block = mm(place_ref[...], block).astype(bf16)
        for e in range(sources):
            to = e * height + k * most
            out_ref[to : to + most, :] = block[e * most : (e + 1) * most]
        rows.append(jnp.sum(own[:, cut] * logit_grad, axis=0, keepdims=True))
    extra = stacked_rows(rows, EXTRA).astype(bf16)
    for e in range(sources):
        out_ref[(e + 1) * height - BACK : (e + 1) * height, :] = extra[0, :BACK]


def finish_kernel(recv_ref, pick_ref, grad_ref, router_ref, got_ref):
    experts = router_ref.shape[0]
    most = pick_ref.shape[0] // experts
    height = recv_ref.shape[0] // experts
    blocks = grad_ref.shape[1] // LANES
    for e in range(experts):
        extra = recv_ref[(e + 1) * height - BACK : (e + 1) * height, :].astype(f32)
        for k in range(blocks):
            cut = slice(k * LANES, (k + 1) * LANES)
            at = e * height + k * most
            got_ref[e * most : (e + 1) * most, cut] = recv_ref[at : at + most, :]
            router_ref[e : e + 1, cut] = extra[k : k + 1]
    grad_ref[...] = mm(pick_ref[...], got_ref[...], ((0,), (0,)))


def exchanged(x, axis):
    shape = (lax.axis_size(axis), -1, 2, LANES)
    return lax.all_to_all(x.reshape(shape), axis, 0, 0, tiled=True).reshape(x.shape)


def kernel_call(body, outs, scalars, *args, flops=0, space=pltpu.VMEM, scratch=()):
    vmem = pl.BlockSpec(memory_space=pltpu.VMEM)
    smem = pl.BlockSpec(memory_space=pltpu.SMEM)
    held = pl.BlockSpec(memory_space=space)
    shapes = [jax.ShapeDtypeStruct(s, t) for s, t in outs]
    return pl.pallas_call(
        body,
        out_shape=shapes,
        in_specs=[smem] * scalars + [held] * (len(args) - scalars),
        out_specs=[vmem] * len(shapes),
        scratch_shapes=list(scratch),
        cost_estimate=pl.CostEstimate(flops=flops, transcendentals=0, bytes_accessed=0) if flops else None,
        compiler_params=pltpu.CompilerParams(vmem_limit_bytes=SCOPED),
    )(*args)


def ring_gather(x, axis):
    n = lax.axis_size(axis)
    up = [(k, (k + 1) % n) for k in range(n)]
    down = [(k, (k - 1) % n) for k in range(n)]
    chunks, offsets = [x], [0]
    right = left = x
    for step in range(1, n // 2 + 1):
        left = lax.ppermute(left, axis, down)
        chunks.append(left)
        offsets.append(step)
        if 2 * step < n:
            right = lax.ppermute(right, axis, up)
            chunks.append(right)
            offsets.append(-step)
    return chunks, tuple(offsets)


def per_device(tokens_in, out_grad, logits, indices, w_in, w_out, router_w):
    tok, cols = tokens_in.shape
    experts, capacity = indices.shape
    most = min(tok, 2 * capacity // experts)
    spread = experts * most
    devices = lax.axis_size("mp")
    blocks = cols // LANES
    given = (indices, tokens_in, out_grad, logits.T)
    stored = (w_in[0], w_out[0])
    send, pick, own, *weights = kernel_call(
        pack_kernel,
        [
            ((experts * (2 * blocks * most + SENT), LANES), bf16),
            ((spread, tok), bf16),
            ((1, capacity), i32),
            *((w.shape, w.dtype) for w in stored),
        ],
        0,
        *(pltpu.with_memory_space_constraint(x, pltpu.HBM) for x in given + stored),
        space=pltpu.HBM,
        scratch=[pltpu.VMEM(x.shape, x.dtype) for x in given] + [pltpu.SemaphoreType.DMA((6,))],
    )
    recv = exchanged(send, "expert")
    rows, probs, place_back = kernel_call(
        functools.partial(compact_kernel, tok=tok),
        [((capacity, 2 * cols), bf16), ((capacity, LANES), f32), ((spread, capacity), bf16)],
        0,
        own,
        recv,
        scratch=[pltpu.VMEM((spread, 2 * cols), bf16), pltpu.VMEM((SENT, experts, LANES), f32)],
    )
    chunks, offsets = ring_gather(rows, "mp")
    hidden = w_in.shape[2]
    early = len(chunks) - 1
    pre, back = kernel_call(
        functools.partial(first_kernel, offsets=offsets[:early], devices=devices),
        [((capacity, hidden), f32)] * 2,
        0,
        *chunks[:early],
        *weights,
        flops=4 * early * capacity * cols * hidden,
    )
    (parts,) = kernel_call(
        functools.partial(hidden_kernel, offsets=offsets[early:]),
        [((devices, blocks * capacity + EXTRA, LANES), bf16)],
        0,
        pre,
        back,
        *chunks[early:],
        *weights,
    )
    parts = lax.all_to_all(parts, "mp", 0, 0, tiled=True)
    (back,) = kernel_call(
        combine_kernel,
        [((experts * (blocks * most + BACK), LANES), bf16)],
        0,
        parts,
        probs,
        rows,
        router_w.T,
        place_back,
    )
    back = exchanged(back, "expert")
    input_grad, router_grad = kernel_call(
        finish_kernel,
        [((tok, cols), f32), ((experts, cols), f32)],
        0,
        back,
        pick,
        scratch=[pltpu.VMEM((spread, cols), bf16)],
    )
    return input_grad, router_grad.T


def solution(mesh):
    return jax.shard_map(
        per_device,
        mesh=mesh,
        in_specs=(
            P(("groups", "expert"), "mp"),
            P(("groups", "expert"), "mp"),
            P(("groups", "expert"), None),
            P("groups", None),
            P("expert", None, "mp"),
            P("expert", "mp", None),
            P("mp", None),
        ),
        out_specs=(P(("groups", "expert"), "mp"), P(("groups", "mp"), None)),
        check_vma=False,
    )
```

```python
import functools

import jax
import jax.numpy as jnp
from jax import lax
from jax.experimental import pallas as pl
from jax.experimental.pallas import tpu as pltpu
from jax.sharding import PartitionSpec as P


inv_root_two = 0.7071067811865476
inv_root_tau = 0.3989422804014327
LANES = 128
EXTRA = 8
SENT = 4
BACK = 2
SCOPED = 16 * 2**20
f32 = jnp.float32
bf16 = jnp.bfloat16
i32 = jnp.int32


def mm(a, b, contract=((1,), (0,))):
    return lax.dot_general(a, b, (contract, ((), ())), preferred_element_type=f32)


def iota(shape, dim):
    return lax.broadcasted_iota(i32, shape, dim)


def in_parts(v, parts):
    out = []
    for _ in range(parts):
        part = v.astype(bf16).astype(f32)
        out.append(part)
        v = v - part
    return out


def row_to_column(row):
    n = row.shape[1]
    eye = iota((n, n), 0) == iota((n, n), 1)
    return jnp.sum(jnp.where(eye, row, jnp.zeros_like(row)), axis=1, keepdims=True)


def column_to_row(column):
    n = column.shape[0]
    eye = iota((n, n), 0) == iota((n, n), 1)
    return jnp.sum(jnp.where(eye, column, jnp.zeros_like(column)), axis=0, keepdims=True)


def stacked_rows(rows, height):
    count = rows[0].shape[0]
    at = iota((count, height, LANES), 1)
    out = jnp.zeros((count, height, LANES), f32)
    for k, row in enumerate(rows):
        out = jnp.where(at == k, row[:, None, :], out)
    return out


def pack_kernel(*refs):
    given, (send_ref, pick_ref, own_ref), held, done = refs[:6], refs[6:9], refs[11:15], refs[15]
    held += refs[9:11]
    copies = [pltpu.make_async_copy(a, b, done.at[k]) for k, (a, b) in enumerate(zip(given, held))]
    for copy in copies:
        copy.start()
    idx_ref, tok_ref, grad_ref, logit_ref = held[:4]
    copies[0].wait()
    own_ref[...] = idx_ref[pl.ds(lax.axis_index("expert"), 1), :]
    experts, capacity = idx_ref.shape
    tok, cols = tok_ref.shape
    most = pick_ref.shape[0] // experts
    local = idx_ref[...] - lax.axis_index("expert") * tok
    mine = jnp.where((local >= 0) & (local < tok), 1.0, 0.0)
    before = (iota((capacity, capacity), 0) < iota((capacity, capacity), 1)).astype(f32)
    rank = mm(mine.astype(bf16), before.astype(bf16))
    rank = jnp.where(mine > 0.0, rank, -1.0)
    local = (local + 1).astype(f32)
    ranks = iota((most, capacity), 0).astype(f32)
    tokens = iota((most, tok), 1).astype(f32) + 1.0
    for e in range(experts):
        chosen = jnp.where(rank[e : e + 1] == ranks, local[e : e + 1], 0.0)
        chosen = jnp.sum(chosen, axis=1, keepdims=True)
        hit = jnp.where(chosen == tokens, 1.0, 0.0)
        pick_ref[e * most : (e + 1) * most, :] = hit.astype(bf16)
    pick = pick_ref[...]
    height = send_ref.shape[0] // experts
    at = 0
    for ref, copy in ((tok_ref, copies[1]), (grad_ref, copies[2])):
        copy.wait()
        rows = mm(pick, ref[...]).astype(bf16)
        for k in range(0, cols, LANES):
            for e in range(experts):
                to = e * height + at
                send_ref[to : to + most, :] = rows[e * most : (e + 1) * most, k : k + LANES]
            at += most
    copies[3].wait()
    rows = []
    for part in in_parts(logit_ref[...], 2):
        rows += [part[:, k : k + LANES] for k in range(0, tok, LANES)]
    extra = stacked_rows(rows, EXTRA).astype(bf16)
    for e in range(experts):
        to = e * height + at
        send_ref[to : to + SENT, :] = extra[e, :SENT]
    for copy in copies[4:]:
        copy.wait()


def compact_kernel(own_ref, recv_ref, rows_ref, probs_ref, target_ref, got_ref, extra_ref, *, tok):
    capacity, spread = rows_ref.shape[0], got_ref.shape[0]
    sources = extra_ref.shape[1]
    most = spread // sources
    square = (capacity, capacity)
    own_row = own_ref[...]
    own_col = row_to_column(own_row)
    key_row = own_row // tok * capacity + iota((1, capacity), 1)
    key_col = own_col // tok * capacity + iota((capacity, 1), 0)
    pos_row = jnp.sum((key_col < key_row).astype(i32), axis=0, keepdims=True)
    token = jnp.sum(jnp.where(pos_row == iota(square, 0), own_row, 0), axis=1, keepdims=True)
    src = token // tok
    local = token - src * tok
    wide = (capacity, LANES)
    start = jnp.sum((own_col < iota(wide, 1) * tok).astype(i32), axis=0, keepdims=True)
    first = jnp.sum(jnp.where(src == iota(wide, 1), start, 0), axis=1, keepdims=True)
    target = src * most + iota((capacity, 1), 0) - first
    place = jnp.where(target == iota((capacity, spread), 1), 1.0, 0.0).astype(bf16)
    target_ref[...] = jnp.broadcast_to(target, wide)
    pick = jnp.where(src == iota((capacity, sources), 1), 1.0, 0.0).astype(bf16)
    height = recv_ref.shape[0] // sources
    blocks = rows_ref.shape[1] // LANES
    for e in range(sources):
        for k in range(blocks):
            at = e * height + k * most
            got_ref[e * most : (e + 1) * most, k * LANES : (k + 1) * LANES] = recv_ref[
                at : at + most, :
            ]
        extra = recv_ref[e * height + blocks * most : (e + 1) * height, :].astype(f32)
        for k in range(SENT):
            extra_ref[k, e : e + 1, :] = extra[k : k + 1]
    rows_ref[...] = mm(place, got_ref[...]).astype(bf16)
    lanes = iota(wide, 1)
    per = SENT // 2
    logits = jnp.zeros((capacity, 1), f32)
    for k in range(per):
        table = mm(pick, extra_ref[k].astype(bf16)) + mm(pick, extra_ref[per + k].astype(bf16))
        hit = lanes + k * LANES == local
        logits = logits + jnp.sum(jnp.where(hit, table, 0.0), axis=1, keepdims=True)
    probs_ref[...] = jax.nn.sigmoid(jnp.broadcast_to(logits, (capacity, LANES)))


def products(chunks, offsets, win_ref, wout_ref, devices, pre=None, back=None):
    cols = win_ref.shape[0] // devices
    for chunk, offset in zip(chunks, offsets):
        block = lax.rem(lax.axis_index("mp") + offset + devices, devices)
        span = pl.ds(pl.multiple_of(block * cols, cols), cols)
        one = mm(chunk[:, :cols], win_ref[span, :])
        two = mm(chunk[:, cols:], wout_ref[:, span], ((1,), (1,)))
        pre = one if pre is None else pre + one
        back = two if back is None else back + two
    return pre, back


def first_kernel(*refs, offsets, devices):
    chunks = refs[: len(offsets)]
    win_ref, wout_ref, target_ref, pre_ref, back_ref, place_ref = refs[len(offsets) :]
    target = column_to_row(target_ref[:, :1])
    place = jnp.where(target == iota(place_ref.shape, 0), 1.0, 0.0)
    place_ref[...] = place.astype(bf16)
    pre_ref[...], back_ref[...] = products(
        chunks, offsets, win_ref, wout_ref, devices
    )


def hidden_kernel(pre_ref, back_ref, *refs, offsets):
    chunks = refs[: len(offsets)]
    win_ref, wout_ref, out_ref = refs[len(offsets) :]
    devices = out_ref.shape[0]
    capacity, both = chunks[0].shape
    cols = both // 2
    pre, back = products(
        chunks, offsets, win_ref, wout_ref, devices, pre_ref[...], back_ref[...]
    )
    cumulative = 0.5 * (1.0 + lax.erf(pre * inv_root_two))
    slopes = cumulative + pre * jnp.exp(-0.5 * pre * pre) * inv_root_tau
    gates = jnp.sum(pre * cumulative * back, axis=1, keepdims=True)
    delta = (back * slopes).astype(bf16)
    for d in range(devices):
        block = mm(delta, win_ref[d * cols : (d + 1) * cols, :], ((1,), (1,))).astype(bf16)
        for k in range(cols // LANES):
            out_ref[d, k * capacity : (k + 1) * capacity, :] = block[:, k * LANES : (k + 1) * LANES]
    gates = column_to_row(gates)
    rows = []
    for part in in_parts(gates, 3):
        rows += [part[:, k : k + LANES] for k in range(0, capacity, LANES)]
    extra = stacked_rows(rows, EXTRA).astype(bf16)
    at = cols // LANES * capacity
    out_ref[:, at : at + EXTRA, :] = jnp.broadcast_to(extra, (devices, EXTRA, LANES))


def combine_kernel(parts_ref, probs_ref, own_ref, router_ref, place_ref, out_ref):
    devices = parts_ref.shape[0]
    capacity, both = own_ref.shape
    cols = both // 2
    blocks = cols // LANES
    sources = router_ref.shape[0]
    most = place_ref.shape[0] // sources
    height = out_ref.shape[0] // sources
    at = blocks * capacity
    extra = jnp.sum(parts_ref[:, at : at + EXTRA, :].astype(f32), axis=0)
    per = capacity // LANES
    gates = extra[:per] + extra[per : 2 * per] + extra[2 * per : 3 * per]
    gates = jnp.concatenate([row_to_column(gates[k : k + 1]) for k in range(per)], axis=0)
    probs = probs_ref[...]
    logit_grad = (probs * (1.0 - probs) * gates).astype(bf16).astype(f32)
    router = router_ref[...].astype(f32)
    mine = iota(router.shape, 0) == lax.axis_index("expert")
    router = jnp.sum(jnp.where(mine, router, 0.0), axis=0, keepdims=True)
    rows, own = [], own_ref[:, :cols].astype(f32)
    for k in range(blocks):
        total = jnp.zeros((capacity, LANES), f32)
        for d in range(devices):
            total = total + parts_ref[d, k * capacity : (k + 1) * capacity, :].astype(f32)
        cut = slice(k * LANES, (k + 1) * LANES)
        block = (total * probs + logit_grad * router[:, cut]).astype(bf16)
        block = mm(place_ref[...], block).astype(bf16)
        for e in range(sources):
            to = e * height + k * most
            out_ref[to : to + most, :] = block[e * most : (e + 1) * most]
        rows.append(jnp.sum(own[:, cut] * logit_grad, axis=0, keepdims=True))
    extra = stacked_rows(rows, EXTRA).astype(bf16)
    for e in range(sources):
        out_ref[(e + 1) * height - BACK : (e + 1) * height, :] = extra[0, :BACK]


def finish_kernel(recv_ref, pick_ref, grad_ref, router_ref, got_ref):
    experts = router_ref.shape[0]
    most = pick_ref.shape[0] // experts
    height = recv_ref.shape[0] // experts
    blocks = grad_ref.shape[1] // LANES
    for e in range(experts):
        extra = recv_ref[(e + 1) * height - BACK : (e + 1) * height, :].astype(f32)
        for k in range(blocks):
            cut = slice(k * LANES, (k + 1) * LANES)
            at = e * height + k * most
            got_ref[e * most : (e + 1) * most, cut] = recv_ref[at : at + most, :]
            router_ref[e : e + 1, cut] = extra[k : k + 1]
    grad_ref[...] = mm(pick_ref[...], got_ref[...], ((0,), (0,)))


def exchanged(x, axis):
    shape = (lax.axis_size(axis), -1, 2, LANES)
    return lax.all_to_all(x.reshape(shape), axis, 0, 0, tiled=True).reshape(x.shape)


def kernel_call(body, outs, scalars, *args, flops=0, space=pltpu.VMEM, scratch=()):
    vmem = pl.BlockSpec(memory_space=pltpu.VMEM)
    smem = pl.BlockSpec(memory_space=pltpu.SMEM)
    held = pl.BlockSpec(memory_space=space)
    shapes = [jax.ShapeDtypeStruct(s, t) for s, t in outs]
    return pl.pallas_call(
        body,
        out_shape=shapes,
        in_specs=[smem] * scalars + [held] * (len(args) - scalars),
        out_specs=[vmem] * len(shapes),
        scratch_shapes=list(scratch),
        cost_estimate=pl.CostEstimate(flops=flops, transcendentals=0, bytes_accessed=0) if flops else None,
        compiler_params=pltpu.CompilerParams(vmem_limit_bytes=SCOPED),
    )(*args)


def ring_gather(x, axis):
    n = lax.axis_size(axis)
    up = [(k, (k + 1) % n) for k in range(n)]
    down = [(k, (k - 1) % n) for k in range(n)]
    chunks, offsets = [x], [0]
    right = left = x
    for step in range(1, n // 2 + 1):
        left = lax.ppermute(left, axis, down)
        chunks.append(left)
        offsets.append(step)
        if 2 * step < n:
            right = lax.ppermute(right, axis, up)
            chunks.append(right)
            offsets.append(-step)
    return chunks, tuple(offsets)


def per_device(tokens_in, out_grad, logits, indices, w_in, w_out, router_w):
    tok, cols = tokens_in.shape
    experts, capacity = indices.shape
    most = min(tok, 2 * capacity // experts)
    spread = experts * most
    devices = lax.axis_size("mp")
    blocks = cols // LANES
    given = (indices, tokens_in, out_grad, logits.T)
    stored = (w_in[0], w_out[0])
    send, pick, own, *weights = kernel_call(
        pack_kernel,
        [
            ((experts * (2 * blocks * most + SENT), LANES), bf16),
            ((spread, tok), bf16),
            ((1, capacity), i32),
            *((w.shape, w.dtype) for w in stored),
        ],
        0,
        *(pltpu.with_memory_space_constraint(x, pltpu.HBM) for x in given + stored),
        space=pltpu.HBM,
        scratch=[pltpu.VMEM(x.shape, x.dtype) for x in given] + [pltpu.SemaphoreType.DMA((6,))],
    )
    recv = exchanged(send, "expert")
    rows, probs, target = kernel_call(
        functools.partial(compact_kernel, tok=tok),
        [((capacity, 2 * cols), bf16), ((capacity, LANES), f32), ((capacity, LANES), i32)],
        0,
        own,
        recv,
        scratch=[pltpu.VMEM((spread, 2 * cols), bf16), pltpu.VMEM((SENT, experts, LANES), f32)],
    )
    chunks, offsets = ring_gather(rows, "mp")
    hidden = w_in.shape[2]
    early = len(chunks) - 1
    pre, back, place_back = kernel_call(
        functools.partial(first_kernel, offsets=offsets[:early], devices=devices),
        [((capacity, hidden), f32)] * 2 + [((spread, capacity), bf16)],
        0,
        *chunks[:early],
        *weights,
        target,
        flops=4 * early * capacity * cols * hidden,
    )
    (parts,) = kernel_call(
        functools.partial(hidden_kernel, offsets=offsets[early:]),
        [((devices, blocks * capacity + EXTRA, LANES), bf16)],
        0,
        pre,
        back,
        *chunks[early:],
        *weights,
    )
    parts = lax.all_to_all(parts, "mp", 0, 0, tiled=True)
    (back,) = kernel_call(
        combine_kernel,
        [((experts * (blocks * most + BACK), LANES), bf16)],
        0,
        parts,
        probs,
        rows,
        router_w.T,
        place_back,
    )
    back = exchanged(back, "expert")
    input_grad, router_grad = kernel_call(
        finish_kernel,
        [((tok, cols), f32), ((experts, cols), f32)],
        0,
        back,
        pick,
        scratch=[pltpu.VMEM((spread, cols), bf16)],
    )
    return input_grad, router_grad.T


def solution(mesh):
    return jax.shard_map(
        per_device,
        mesh=mesh,
        in_specs=(
            P(("groups", "expert"), "mp"),
            P(("groups", "expert"), "mp"),
            P(("groups", "expert"), None),
            P("groups", None),
            P("expert", None, "mp"),
            P("expert", "mp", None),
            P("mp", None),
        ),
        out_specs=(P(("groups", "expert"), "mp"), P(("groups", "mp"), None)),
        check_vma=False,
    )
```

```python
import functools

import jax
import jax.numpy as jnp
from jax import lax
from jax.experimental import pallas as pl
from jax.experimental.pallas import tpu as pltpu
from jax.sharding import PartitionSpec as P


inv_root_two = 0.7071067811865476
inv_root_tau = 0.3989422804014327
LANES = 128
EXTRA = 8
SENT = 4
BACK = 2
SCOPED = 16 * 2**20
f32 = jnp.float32
bf16 = jnp.bfloat16
i32 = jnp.int32


def mm(a, b, contract=((1,), (0,))):
    return lax.dot_general(a, b, (contract, ((), ())), preferred_element_type=f32)


def iota(shape, dim):
    return lax.broadcasted_iota(i32, shape, dim)


def in_parts(v, parts):
    out = []
    for _ in range(parts):
        part = v.astype(bf16).astype(f32)
        out.append(part)
        v = v - part
    return out


def row_to_column(row):
    n = row.shape[1]
    eye = iota((n, n), 0) == iota((n, n), 1)
    return jnp.sum(jnp.where(eye, row, jnp.zeros_like(row)), axis=1, keepdims=True)


def column_to_row(column):
    n = column.shape[0]
    eye = iota((n, n), 0) == iota((n, n), 1)
    return jnp.sum(jnp.where(eye, column, jnp.zeros_like(column)), axis=0, keepdims=True)


def stacked_rows(rows, height):
    count = rows[0].shape[0]
    at = iota((count, height, LANES), 1)
    out = jnp.zeros((count, height, LANES), f32)
    for k, row in enumerate(rows):
        out = jnp.where(at == k, row[:, None, :], out)
    return out


def pack_kernel(*refs):
    given, (send_ref, pick_ref, own_ref), held, done = refs[:4], refs[4:7], refs[7:11], refs[11]
    copies = [pltpu.make_async_copy(a, b, done.at[k]) for k, (a, b) in enumerate(zip(given, held))]
    for copy in copies:
        copy.start()
    idx_ref, tok_ref, grad_ref, logit_ref = held
    copies[0].wait()
    own_ref[...] = idx_ref[pl.ds(lax.axis_index("expert"), 1), :]
    experts, capacity = idx_ref.shape
    tok, cols = tok_ref.shape
    most = pick_ref.shape[0] // experts
    local = idx_ref[...] - lax.axis_index("expert") * tok
    mine = jnp.where((local >= 0) & (local < tok), 1.0, 0.0)
    before = (iota((capacity, capacity), 0) < iota((capacity, capacity), 1)).astype(f32)
    rank = mm(mine.astype(bf16), before.astype(bf16))
    rank = jnp.where(mine > 0.0, rank, -1.0)
    local = (local + 1).astype(f32)
    ranks = iota((most, capacity), 0).astype(f32)
    tokens = iota((most, tok), 1).astype(f32) + 1.0
    for e in range(experts):
        chosen = jnp.where(rank[e : e + 1] == ranks, local[e : e + 1], 0.0)
        chosen = jnp.sum(chosen, axis=1, keepdims=True)
        hit = jnp.where(chosen == tokens, 1.0, 0.0)
        pick_ref[e * most : (e + 1) * most, :] = hit.astype(bf16)
    pick = pick_ref[...]
    height = send_ref.shape[0] // experts
    at = 0
    for ref, copy in ((tok_ref, copies[1]), (grad_ref, copies[2])):
        copy.wait()
        rows = mm(pick, ref[...]).astype(bf16)
        for k in range(0, cols, LANES):
            for e in range(experts):
                to = e * height + at
                send_ref[to : to + most, :] = rows[e * most : (e + 1) * most, k : k + LANES]
            at += most
    copies[3].wait()
    rows = []
    for part in in_parts(logit_ref[...], 2):
        rows += [part[:, k : k + LANES] for k in range(0, tok, LANES)]
    extra = stacked_rows(rows, EXTRA).astype(bf16)
    for e in range(experts):
        to = e * height + at
        send_ref[to : to + SENT, :] = extra[e, :SENT]


def compact_kernel(
    own_ref, recv_ref, stored_ref, rows_ref, probs_ref, target_ref, win_ref, got_ref, extra_ref, done, *, tok
):
    bring = pltpu.make_async_copy(stored_ref, win_ref, done)
    bring.start()
    capacity, spread = rows_ref.shape[0], got_ref.shape[0]
    sources = extra_ref.shape[1]
    most = spread // sources
    square = (capacity, capacity)
    own_row = own_ref[...]
    own_col = row_to_column(own_row)
    key_row = own_row // tok * capacity + iota((1, capacity), 1)
    key_col = own_col // tok * capacity + iota((capacity, 1), 0)
    pos_row = jnp.sum((key_col < key_row).astype(i32), axis=0, keepdims=True)
    token = jnp.sum(jnp.where(pos_row == iota(square, 0), own_row, 0), axis=1, keepdims=True)
    src = token // tok
    local = token - src * tok
    wide = (capacity, LANES)
    start = jnp.sum((own_col < iota(wide, 1) * tok).astype(i32), axis=0, keepdims=True)
    first = jnp.sum(jnp.where(src == iota(wide, 1), start, 0), axis=1, keepdims=True)
    target = src * most + iota((capacity, 1), 0) - first
    place = jnp.where(target == iota((capacity, spread), 1), 1.0, 0.0).astype(bf16)
    target_ref[...] = jnp.broadcast_to(target, wide)
    pick = jnp.where(src == iota((capacity, sources), 1), 1.0, 0.0).astype(bf16)
    height = recv_ref.shape[0] // sources
    blocks = rows_ref.shape[1] // LANES
    for e in range(sources):
        for k in range(blocks):
            at = e * height + k * most
            got_ref[e * most : (e + 1) * most, k * LANES : (k + 1) * LANES] = recv_ref[
                at : at + most, :
            ]
        extra = recv_ref[e * height + blocks * most : (e + 1) * height, :].astype(f32)
        for k in range(SENT):
            extra_ref[k, e : e + 1, :] = extra[k : k + 1]
    rows_ref[...] = mm(place, got_ref[...]).astype(bf16)
    lanes = iota(wide, 1)
    per = SENT // 2
    logits = jnp.zeros((capacity, 1), f32)
    for k in range(per):
        table = mm(pick, extra_ref[k].astype(bf16)) + mm(pick, extra_ref[per + k].astype(bf16))
        hit = lanes + k * LANES == local
        logits = logits + jnp.sum(jnp.where(hit, table, 0.0), axis=1, keepdims=True)
    probs_ref[...] = jax.nn.sigmoid(jnp.broadcast_to(logits, (capacity, LANES)))
    bring.wait()


def products(chunks, offsets, win_ref, wout_ref, devices, pre=None, back=None):
    cols = win_ref.shape[0] // devices
    for chunk, offset in zip(chunks, offsets):
        block = lax.rem(lax.axis_index("mp") + offset + devices, devices)
        span = pl.ds(pl.multiple_of(block * cols, cols), cols)
        one = mm(chunk[:, :cols], win_ref[span, :])
        two = mm(chunk[:, cols:], wout_ref[:, span], ((1,), (1,)))
        pre = one if pre is None else pre + one
        back = two if back is None else back + two
    return pre, back


def first_kernel(*refs, offsets, devices):
    chunks = refs[: len(offsets)]
    win_ref, target_ref, stored_ref = refs[len(offsets) : len(offsets) + 3]
    pre_ref, back_ref, place_ref, wout_ref, done = refs[len(offsets) + 3 :]
    bring = pltpu.make_async_copy(stored_ref, wout_ref, done)
    bring.start()
    target = column_to_row(target_ref[:, :1])
    place = jnp.where(target == iota(place_ref.shape, 0), 1.0, 0.0)
    place_ref[...] = place.astype(bf16)
    bring.wait()
    pre_ref[...], back_ref[...] = products(
        chunks, offsets, win_ref, wout_ref, devices
    )


def hidden_kernel(pre_ref, back_ref, *refs, offsets):
    chunks = refs[: len(offsets)]
    win_ref, wout_ref, out_ref = refs[len(offsets) :]
    devices = out_ref.shape[0]
    capacity, both = chunks[0].shape
    cols = both // 2
    pre, back = products(
        chunks, offsets, win_ref, wout_ref, devices, pre_ref[...], back_ref[...]
    )
    cumulative = 0.5 * (1.0 + lax.erf(pre * inv_root_two))
    slopes = cumulative + pre * jnp.exp(-0.5 * pre * pre) * inv_root_tau
    gates = jnp.sum(pre * cumulative * back, axis=1, keepdims=True)
    delta = (back * slopes).astype(bf16)
    for d in range(devices):
        block = mm(delta, win_ref[d * cols : (d + 1) * cols, :], ((1,), (1,))).astype(bf16)
        for k in range(cols // LANES):
            out_ref[d, k * capacity : (k + 1) * capacity, :] = block[:, k * LANES : (k + 1) * LANES]
    gates = column_to_row(gates)
    rows = []
    for part in in_parts(gates, 3):
        rows += [part[:, k : k + LANES] for k in range(0, capacity, LANES)]
    extra = stacked_rows(rows, EXTRA).astype(bf16)
    at = cols // LANES * capacity
    out_ref[:, at : at + EXTRA, :] = jnp.broadcast_to(extra, (devices, EXTRA, LANES))


def combine_kernel(parts_ref, probs_ref, own_ref, router_ref, place_ref, out_ref):
    devices = parts_ref.shape[0]
    capacity, both = own_ref.shape
    cols = both // 2
    blocks = cols // LANES
    sources = router_ref.shape[0]
    most = place_ref.shape[0] // sources
    height = out_ref.shape[0] // sources
    at = blocks * capacity
    extra = jnp.sum(parts_ref[:, at : at + EXTRA, :].astype(f32), axis=0)
    per = capacity // LANES
    gates = extra[:per] + extra[per : 2 * per] + extra[2 * per : 3 * per]
    gates = jnp.concatenate([row_to_column(gates[k : k + 1]) for k in range(per)], axis=0)
    probs = probs_ref[...]
    logit_grad = (probs * (1.0 - probs) * gates).astype(bf16).astype(f32)
    router = router_ref[...].astype(f32)
    mine = iota(router.shape, 0) == lax.axis_index("expert")
    router = jnp.sum(jnp.where(mine, router, 0.0), axis=0, keepdims=True)
    rows, own = [], own_ref[:, :cols].astype(f32)
    for k in range(blocks):
        total = jnp.zeros((capacity, LANES), f32)
        for d in range(devices):
            total = total + parts_ref[d, k * capacity : (k + 1) * capacity, :].astype(f32)
        cut = slice(k * LANES, (k + 1) * LANES)
        block = (total * probs + logit_grad * router[:, cut]).astype(bf16)
        block = mm(place_ref[...], block).astype(bf16)
        for e in range(sources):
            to = e * height + k * most
            out_ref[to : to + most, :] = block[e * most : (e + 1) * most]
        rows.append(jnp.sum(own[:, cut] * logit_grad, axis=0, keepdims=True))
    extra = stacked_rows(rows, EXTRA).astype(bf16)
    for e in range(sources):
        out_ref[(e + 1) * height - BACK : (e + 1) * height, :] = extra[0, :BACK]


def finish_kernel(recv_ref, pick_ref, grad_ref, router_ref, got_ref):
    experts = router_ref.shape[0]
    most = pick_ref.shape[0] // experts
    height = recv_ref.shape[0] // experts
    blocks = grad_ref.shape[1] // LANES
    for e in range(experts):
        extra = recv_ref[(e + 1) * height - BACK : (e + 1) * height, :].astype(f32)
        for k in range(blocks):
            cut = slice(k * LANES, (k + 1) * LANES)
            at = e * height + k * most
            got_ref[e * most : (e + 1) * most, cut] = recv_ref[at : at + most, :]
            router_ref[e : e + 1, cut] = extra[k : k + 1]
    grad_ref[...] = mm(pick_ref[...], got_ref[...], ((0,), (0,)))


def exchanged(x, axis):
    shape = (lax.axis_size(axis), -1, 2, LANES)
    return lax.all_to_all(x.reshape(shape), axis, 0, 0, tiled=True).reshape(x.shape)


def kernel_call(body, outs, scalars, *args, flops=0, hbm=0, scratch=()):
    vmem = pl.BlockSpec(memory_space=pltpu.VMEM)
    smem = pl.BlockSpec(memory_space=pltpu.SMEM)
    far = pl.BlockSpec(memory_space=pltpu.HBM)
    shapes = [jax.ShapeDtypeStruct(s, t) for s, t in outs]
    near = len(args) - hbm
    args = args[:near] + tuple(pltpu.with_memory_space_constraint(x, pltpu.HBM) for x in args[near:])
    return pl.pallas_call(
        body,
        out_shape=shapes,
        in_specs=[smem] * scalars + [vmem] * (near - scalars) + [far] * hbm,
        out_specs=[vmem] * len(shapes),
        scratch_shapes=list(scratch),
        cost_estimate=pl.CostEstimate(flops=flops, transcendentals=0, bytes_accessed=0) if flops else None,
        compiler_params=pltpu.CompilerParams(vmem_limit_bytes=SCOPED),
    )(*args)


def ring_gather(x, axis):
    n = lax.axis_size(axis)
    up = [(k, (k + 1) % n) for k in range(n)]
    down = [(k, (k - 1) % n) for k in range(n)]
    chunks, offsets = [x], [0]
    right = left = x
    for step in range(1, n // 2 + 1):
        left = lax.ppermute(left, axis, down)
        chunks.append(left)
        offsets.append(step)
        if 2 * step < n:
            right = lax.ppermute(right, axis, up)
            chunks.append(right)
            offsets.append(-step)
    return chunks, tuple(offsets)


def per_device(tokens_in, out_grad, logits, indices, w_in, w_out, router_w):
    tok, cols = tokens_in.shape
    experts, capacity = indices.shape
    most = min(tok, 2 * capacity // experts)
    spread = experts * most
    devices = lax.axis_size("mp")
    blocks = cols // LANES
    given = (indices, tokens_in, out_grad, logits.T)
    send, pick, own = kernel_call(
        pack_kernel,
        [
            ((experts * (2 * blocks * most + SENT), LANES), bf16),
            ((spread, tok), bf16),
            ((1, capacity), i32),
        ],
        0,
        *given,
        hbm=4,
        scratch=[pltpu.VMEM(x.shape, x.dtype) for x in given] + [pltpu.SemaphoreType.DMA((4,))],
    )
    recv = exchanged(send, "expert")
    rows, probs, target, win = kernel_call(
        functools.partial(compact_kernel, tok=tok),
        [
            ((capacity, 2 * cols), bf16),
            ((capacity, LANES), f32),
            ((capacity, LANES), i32),
            (w_in.shape[1:], bf16),
        ],
        0,
        own,
        recv,
        w_in[0],
        hbm=1,
        scratch=[
            pltpu.VMEM((spread, 2 * cols), bf16),
            pltpu.VMEM((SENT, experts, LANES), f32),
            pltpu.SemaphoreType.DMA,
        ],
    )
    chunks, offsets = ring_gather(rows, "mp")
    hidden = w_in.shape[2]
    early = len(chunks) - 1
    pre, back, place_back, wout = kernel_call(
        functools.partial(first_kernel, offsets=offsets[:early], devices=devices),
        [((capacity, hidden), f32)] * 2 + [((spread, capacity), bf16), (w_out.shape[1:], bf16)],
        0,
        *chunks[:early],
        win,
        target,
        w_out[0],
        hbm=1,
        scratch=[pltpu.SemaphoreType.DMA],
        flops=4 * early * capacity * cols * hidden,
    )
    (parts,) = kernel_call(
        functools.partial(hidden_kernel, offsets=offsets[early:]),
        [((devices, blocks * capacity + EXTRA, LANES), bf16)],
        0,
        pre,
        back,
        *chunks[early:],
        win,
        wout,
    )
    parts = lax.all_to_all(parts, "mp", 0, 0, tiled=True)
    (back,) = kernel_call(
        combine_kernel,
        [((experts * (blocks * most + BACK), LANES), bf16)],
        0,
        parts,
        probs,
        rows,
        router_w.T,
        place_back,
    )
    back = exchanged(back, "expert")
    input_grad, router_grad = kernel_call(
        finish_kernel,
        [((tok, cols), f32), ((experts, cols), f32)],
        0,
        back,
        pick,
        scratch=[pltpu.VMEM((spread, cols), bf16)],
    )
    return input_grad, router_grad.T


def solution(mesh):
    return jax.shard_map(
        per_device,
        mesh=mesh,
        in_specs=(
            P(("groups", "expert"), "mp"),
            P(("groups", "expert"), "mp"),
            P(("groups", "expert"), None),
            P("groups", None),
            P("expert", None, "mp"),
            P("expert", "mp", None),
            P("mp", None),
        ),
        out_specs=(P(("groups", "expert"), "mp"), P(("groups", "mp"), None)),
        check_vma=False,
    )
```

```python
import functools

import jax
import jax.numpy as jnp
from jax import lax
from jax.experimental import pallas as pl
from jax.experimental.pallas import tpu as pltpu
from jax.sharding import PartitionSpec as P


inv_root_two = 0.7071067811865476
inv_root_tau = 0.3989422804014327
LANES = 128
EXTRA = 8
SENT = 4
BACK = 2
SCOPED = 16 * 2**20
f32 = jnp.float32
bf16 = jnp.bfloat16
i32 = jnp.int32


def mm(a, b, contract=((1,), (0,))):
    return lax.dot_general(a, b, (contract, ((), ())), preferred_element_type=f32)


def iota(shape, dim):
    return lax.broadcasted_iota(i32, shape, dim)


def in_parts(v, parts):
    out = []
    for _ in range(parts):
        part = v.astype(bf16).astype(f32)
        out.append(part)
        v = v - part
    return out


def row_to_column(row):
    n = row.shape[1]
    eye = iota((n, n), 0) == iota((n, n), 1)
    return jnp.sum(jnp.where(eye, row, jnp.zeros_like(row)), axis=1, keepdims=True)


def column_to_row(column):
    n = column.shape[0]
    eye = iota((n, n), 0) == iota((n, n), 1)
    return jnp.sum(jnp.where(eye, column, jnp.zeros_like(column)), axis=0, keepdims=True)


def stacked_rows(rows, height):
    count = rows[0].shape[0]
    at = iota((count, height, LANES), 1)
    out = jnp.zeros((count, height, LANES), f32)
    for k, row in enumerate(rows):
        out = jnp.where(at == k, row[:, None, :], out)
    return out


def pack_kernel(*refs):
    given, (send_ref, pick_ref, own_ref), held, done = refs[:4], refs[4:7], refs[7:11], refs[11]
    copies = [pltpu.make_async_copy(a, b, done.at[k]) for k, (a, b) in enumerate(zip(given, held))]
    for copy in copies:
        copy.start()
    idx_ref, tok_ref, grad_ref, logit_ref = held
    copies[0].wait()
    own_ref[...] = idx_ref[pl.ds(lax.axis_index("expert"), 1), :]
    experts, capacity = idx_ref.shape
    tok, cols = tok_ref.shape
    most = pick_ref.shape[0] // experts
    local = idx_ref[...] - lax.axis_index("expert") * tok
    mine = jnp.where((local >= 0) & (local < tok), 1.0, 0.0)
    before = (iota((capacity, capacity), 0) < iota((capacity, capacity), 1)).astype(f32)
    rank = mm(mine.astype(bf16), before.astype(bf16))
    rank = jnp.where(mine > 0.0, rank, -1.0)
    local = (local + 1).astype(f32)
    ranks = iota((most, capacity), 0).astype(f32)
    tokens = iota((most, tok), 1).astype(f32) + 1.0
    for e in range(experts):
        chosen = jnp.where(rank[e : e + 1] == ranks, local[e : e + 1], 0.0)
        chosen = jnp.sum(chosen, axis=1, keepdims=True)
        hit = jnp.where(chosen == tokens, 1.0, 0.0)
        pick_ref[e * most : (e + 1) * most, :] = hit.astype(bf16)
    pick = pick_ref[...]
    height = send_ref.shape[0] // experts
    at = 0
    for ref, copy in ((tok_ref, copies[1]), (grad_ref, copies[2])):
        copy.wait()
        rows = mm(pick, ref[...]).astype(bf16)
        for k in range(0, cols, LANES):
            for e in range(experts):
                to = e * height + at
                send_ref[to : to + most, :] = rows[e * most : (e + 1) * most, k : k + LANES]
            at += most
    copies[3].wait()
    rows = []
    for part in in_parts(logit_ref[...], 2):
        rows += [part[:, k : k + LANES] for k in range(0, tok, LANES)]
    extra = stacked_rows(rows, EXTRA).astype(bf16)
    for e in range(experts):
        to = e * height + at
        send_ref[to : to + SENT, :] = extra[e, :SENT]


def compact_kernel(own_ref, recv_ref, rows_ref, probs_ref, target_ref, got_ref, extra_ref, *, tok):
    capacity, spread = rows_ref.shape[0], got_ref.shape[0]
    sources = extra_ref.shape[1]
    most = spread // sources
    square = (capacity, capacity)
    own_row = own_ref[...]
    own_col = row_to_column(own_row)
    key_row = own_row // tok * capacity + iota((1, capacity), 1)
    key_col = own_col // tok * capacity + iota((capacity, 1), 0)
    pos_row = jnp.sum((key_col < key_row).astype(i32), axis=0, keepdims=True)
    token = jnp.sum(jnp.where(pos_row == iota(square, 0), own_row, 0), axis=1, keepdims=True)
    src = token // tok
    local = token - src * tok
    wide = (capacity, LANES)
    start = jnp.sum((own_col < iota(wide, 1) * tok).astype(i32), axis=0, keepdims=True)
    first = jnp.sum(jnp.where(src == iota(wide, 1), start, 0), axis=1, keepdims=True)
    target = src * most + iota((capacity, 1), 0) - first
    place = jnp.where(target == iota((capacity, spread), 1), 1.0, 0.0).astype(bf16)
    target_ref[...] = jnp.broadcast_to(target, wide)
    pick = jnp.where(src == iota((capacity, sources), 1), 1.0, 0.0).astype(bf16)
    height = recv_ref.shape[0] // sources
    blocks = rows_ref.shape[1] // LANES
    for e in range(sources):
        for k in range(blocks):
            at = e * height + k * most
            got_ref[e * most : (e + 1) * most, k * LANES : (k + 1) * LANES] = recv_ref[
                at : at + most, :
            ]
        extra = recv_ref[e * height + blocks * most : (e + 1) * height, :].astype(f32)
        for k in range(SENT):
            extra_ref[k, e : e + 1, :] = extra[k : k + 1]
    rows_ref[...] = mm(place, got_ref[...]).astype(bf16)
    lanes = iota(wide, 1)
    per = SENT // 2
    logits = jnp.zeros((capacity, 1), f32)
    for k in range(per):
        table = mm(pick, extra_ref[k].astype(bf16)) + mm(pick, extra_ref[per + k].astype(bf16))
        hit = lanes + k * LANES == local
        logits = logits + jnp.sum(jnp.where(hit, table, 0.0), axis=1, keepdims=True)
    probs_ref[...] = jax.nn.sigmoid(jnp.broadcast_to(logits, (capacity, LANES)))


def spans(ref, dim, offsets, devices):
    size = ref.shape[dim] // devices
    out = []
    for offset in offsets:
        block = lax.rem(lax.axis_index("mp") + offset + devices, devices)
        out.append(pl.ds(pl.multiple_of(block * size, size), size))
    return out


def pre_products(chunks, offsets, win_ref, devices):
    cols = win_ref.shape[0] // devices
    at = spans(win_ref, 0, offsets, devices)
    return sum(mm(chunk[:, :cols], win_ref[span, :]) for chunk, span in zip(chunks, at))


def back_products(chunks, offsets, wout_ref, devices):
    cols = wout_ref.shape[1] // devices
    at = spans(wout_ref, 1, offsets, devices)
    return sum(mm(chunk[:, cols:], wout_ref[:, span], ((1,), (1,))) for chunk, span in zip(chunks, at))


def first_kernel(*refs, offsets, devices):
    chunks, refs = refs[: len(offsets)], refs[len(offsets) :]
    target_ref, stored, (pre_ref, back_ref, place_ref), held, done = (
        refs[0], refs[1:3], refs[3:6], refs[6:8], refs[8]
    )
    copies = [pltpu.make_async_copy(a, b, done.at[k]) for k, (a, b) in enumerate(zip(stored, held))]
    for copy in copies:
        copy.start()
    target = column_to_row(target_ref[:, :1])
    place = jnp.where(target == iota(place_ref.shape, 0), 1.0, 0.0)
    place_ref[...] = place.astype(bf16)
    copies[0].wait()
    pre_ref[...] = pre_products(chunks, offsets, held[0], devices)
    copies[1].wait()
    back_ref[...] = back_products(chunks, offsets, held[1], devices)


def hidden_kernel(pre_ref, back_ref, *refs, offsets):
    chunks = refs[: len(offsets)]
    win_ref, wout_ref, out_ref = refs[len(offsets) :]
    devices = out_ref.shape[0]
    capacity, both = chunks[0].shape
    cols = both // 2
    pre = pre_ref[...] + pre_products(chunks, offsets, win_ref, devices)
    back = back_ref[...] + back_products(chunks, offsets, wout_ref, devices)
    cumulative = 0.5 * (1.0 + lax.erf(pre * inv_root_two))
    slopes = cumulative + pre * jnp.exp(-0.5 * pre * pre) * inv_root_tau
    gates = jnp.sum(pre * cumulative * back, axis=1, keepdims=True)
    delta = (back * slopes).astype(bf16)
    for d in range(devices):
        block = mm(delta, win_ref[d * cols : (d + 1) * cols, :], ((1,), (1,))).astype(bf16)
        for k in range(cols // LANES):
            out_ref[d, k * capacity : (k + 1) * capacity, :] = block[:, k * LANES : (k + 1) * LANES]
    gates = column_to_row(gates)
    rows = []
    for part in in_parts(gates, 3):
        rows += [part[:, k : k + LANES] for k in range(0, capacity, LANES)]
    extra = stacked_rows(rows, EXTRA).astype(bf16)
    at = cols // LANES * capacity
    out_ref[:, at : at + EXTRA, :] = jnp.broadcast_to(extra, (devices, EXTRA, LANES))


def combine_kernel(parts_ref, probs_ref, own_ref, router_ref, place_ref, out_ref):
    devices = parts_ref.shape[0]
    capacity, both = own_ref.shape
    cols = both // 2
    blocks = cols // LANES
    sources = router_ref.shape[0]
    most = place_ref.shape[0] // sources
    height = out_ref.shape[0] // sources
    at = blocks * capacity
    extra = jnp.sum(parts_ref[:, at : at + EXTRA, :].astype(f32), axis=0)
    per = capacity // LANES
    gates = extra[:per] + extra[per : 2 * per] + extra[2 * per : 3 * per]
    gates = jnp.concatenate([row_to_column(gates[k : k + 1]) for k in range(per)], axis=0)
    probs = probs_ref[...]
    logit_grad = (probs * (1.0 - probs) * gates).astype(bf16).astype(f32)
    router = router_ref[...].astype(f32)
    mine = iota(router.shape, 0) == lax.axis_index("expert")
    router = jnp.sum(jnp.where(mine, router, 0.0), axis=0, keepdims=True)
    rows, own = [], own_ref[:, :cols].astype(f32)
    for k in range(blocks):
        total = jnp.zeros((capacity, LANES), f32)
        for d in range(devices):
            total = total + parts_ref[d, k * capacity : (k + 1) * capacity, :].astype(f32)
        cut = slice(k * LANES, (k + 1) * LANES)
        block = (total * probs + logit_grad * router[:, cut]).astype(bf16)
        block = mm(place_ref[...], block).astype(bf16)
        for e in range(sources):
            to = e * height + k * most
            out_ref[to : to + most, :] = block[e * most : (e + 1) * most]
        rows.append(jnp.sum(own[:, cut] * logit_grad, axis=0, keepdims=True))
    extra = stacked_rows(rows, EXTRA).astype(bf16)
    for e in range(sources):
        out_ref[(e + 1) * height - BACK : (e + 1) * height, :] = extra[0, :BACK]


def finish_kernel(recv_ref, pick_ref, grad_ref, router_ref, got_ref):
    experts = router_ref.shape[0]
    most = pick_ref.shape[0] // experts
    height = recv_ref.shape[0] // experts
    blocks = grad_ref.shape[1] // LANES
    for e in range(experts):
        extra = recv_ref[(e + 1) * height - BACK : (e + 1) * height, :].astype(f32)
        for k in range(blocks):
            cut = slice(k * LANES, (k + 1) * LANES)
            at = e * height + k * most
            got_ref[e * most : (e + 1) * most, cut] = recv_ref[at : at + most, :]
            router_ref[e : e + 1, cut] = extra[k : k + 1]
    grad_ref[...] = mm(pick_ref[...], got_ref[...], ((0,), (0,)))


def exchanged(x, axis):
    shape = (lax.axis_size(axis), -1, 2, LANES)
    return lax.all_to_all(x.reshape(shape), axis, 0, 0, tiled=True).reshape(x.shape)


def kernel_call(body, outs, scalars, *args, flops=0, hbm=0, scratch=()):
    vmem = pl.BlockSpec(memory_space=pltpu.VMEM)
    smem = pl.BlockSpec(memory_space=pltpu.SMEM)
    far = pl.BlockSpec(memory_space=pltpu.HBM)
    shapes = [jax.ShapeDtypeStruct(s, t) for s, t in outs]
    near = len(args) - hbm
    args = args[:near] + tuple(pltpu.with_memory_space_constraint(x, pltpu.HBM) for x in args[near:])
    return pl.pallas_call(
        body,
        out_shape=shapes,
        in_specs=[smem] * scalars + [vmem] * (near - scalars) + [far] * hbm,
        out_specs=[vmem] * len(shapes),
        scratch_shapes=list(scratch),
        cost_estimate=pl.CostEstimate(flops=flops, transcendentals=0, bytes_accessed=0) if flops else None,
        compiler_params=pltpu.CompilerParams(vmem_limit_bytes=SCOPED),
    )(*args)


def ring_gather(x, axis):
    n = lax.axis_size(axis)
    up = [(k, (k + 1) % n) for k in range(n)]
    down = [(k, (k - 1) % n) for k in range(n)]
    chunks, offsets = [x], [0]
    right = left = x
    for step in range(1, n // 2 + 1):
        left = lax.ppermute(left, axis, down)
        chunks.append(left)
        offsets.append(step)
        if 2 * step < n:
            right = lax.ppermute(right, axis, up)
            chunks.append(right)
            offsets.append(-step)
    return chunks, tuple(offsets)


def per_device(tokens_in, out_grad, logits, indices, w_in, w_out, router_w):
    tok, cols = tokens_in.shape
    experts, capacity = indices.shape
    most = min(tok, 2 * capacity // experts)
    spread = experts * most
    devices = lax.axis_size("mp")
    blocks = cols // LANES
    given = (indices, tokens_in, out_grad, logits.T)
    send, pick, own = kernel_call(
        pack_kernel,
        [
            ((experts * (2 * blocks * most + SENT), LANES), bf16),
            ((spread, tok), bf16),
            ((1, capacity), i32),
        ],
        0,
        *given,
        hbm=4,
        scratch=[pltpu.VMEM(x.shape, x.dtype) for x in given] + [pltpu.SemaphoreType.DMA((4,))],
    )
    recv = exchanged(send, "expert")
    rows, probs, target = kernel_call(
        functools.partial(compact_kernel, tok=tok),
        [((capacity, 2 * cols), bf16), ((capacity, LANES), f32), ((capacity, LANES), i32)],
        0,
        own,
        recv,
        scratch=[pltpu.VMEM((spread, 2 * cols), bf16), pltpu.VMEM((SENT, experts, LANES), f32)],
    )
    chunks, offsets = ring_gather(rows, "mp")
    hidden = w_in.shape[2]
    early = len(chunks) - 1
    pre, back, place_back, win, wout = kernel_call(
        functools.partial(first_kernel, offsets=offsets[:early], devices=devices),
        [((capacity, hidden), f32)] * 2
        + [((spread, capacity), bf16), (w_in.shape[1:], bf16), (w_out.shape[1:], bf16)],
        0,
        *chunks[:early],
        target,
        w_in[0],
        w_out[0],
        hbm=2,
        scratch=[pltpu.SemaphoreType.DMA((2,))],
        flops=4 * early * capacity * cols * hidden,
    )
    (parts,) = kernel_call(
        functools.partial(hidden_kernel, offsets=offsets[early:]),
        [((devices, blocks * capacity + EXTRA, LANES), bf16)],
        0,
        pre,
        back,
        *chunks[early:],
        win,
        wout,
    )
    parts = lax.all_to_all(parts, "mp", 0, 0, tiled=True)
    (back,) = kernel_call(
        combine_kernel,
        [((experts * (blocks * most + BACK), LANES), bf16)],
        0,
        parts,
        probs,
        rows,
        router_w.T,
        place_back,
    )
    back = exchanged(back, "expert")
    input_grad, router_grad = kernel_call(
        finish_kernel,
        [((tok, cols), f32), ((experts, cols), f32)],
        0,
        back,
        pick,
        scratch=[pltpu.VMEM((spread, cols), bf16)],
    )
    return input_grad, router_grad.T


def solution(mesh):
    return jax.shard_map(
        per_device,
        mesh=mesh,
        in_specs=(
            P(("groups", "expert"), "mp"),
            P(("groups", "expert"), "mp"),
            P(("groups", "expert"), None),
            P("groups", None),
            P("expert", None, "mp"),
            P("expert", "mp", None),
            P("mp", None),
        ),
        out_specs=(P(("groups", "expert"), "mp"), P(("groups", "mp"), None)),
        check_vma=False,
    )
```

```python
import functools

import jax
import jax.numpy as jnp
from jax import lax
from jax.experimental import pallas as pl
from jax.experimental.pallas import tpu as pltpu
from jax.sharding import PartitionSpec as P


inv_root_two = 0.7071067811865476
inv_root_tau = 0.3989422804014327
LANES = 128
EXTRA = 8
SENT = 4
BACK = 2
SCOPED = 16 * 2**20
f32 = jnp.float32
bf16 = jnp.bfloat16
i32 = jnp.int32


def mm(a, b, contract=((1,), (0,))):
    return lax.dot_general(a, b, (contract, ((), ())), preferred_element_type=f32)


def iota(shape, dim):
    return lax.broadcasted_iota(i32, shape, dim)


def in_parts(v, parts):
    out = []
    for _ in range(parts):
        part = v.astype(bf16).astype(f32)
        out.append(part)
        v = v - part
    return out


def row_to_column(row):
    n = row.shape[1]
    eye = iota((n, n), 0) == iota((n, n), 1)
    return jnp.sum(jnp.where(eye, row, jnp.zeros_like(row)), axis=1, keepdims=True)


def column_to_row(column):
    n = column.shape[0]
    eye = iota((n, n), 0) == iota((n, n), 1)
    return jnp.sum(jnp.where(eye, column, jnp.zeros_like(column)), axis=0, keepdims=True)


def stacked_rows(rows, height):
    count = rows[0].shape[0]
    at = iota((count, height, LANES), 1)
    out = jnp.zeros((count, height, LANES), f32)
    for k, row in enumerate(rows):
        out = jnp.where(at == k, row[:, None, :], out)
    return out


def pack_kernel(*refs):
    given, (send_ref, pick_ref, own_ref), held, done = refs[:4], refs[4:7], refs[7:11], refs[11]
    copies = [pltpu.make_async_copy(a, b, done.at[k]) for k, (a, b) in enumerate(zip(given, held))]
    for copy in copies:
        copy.start()
    idx_ref, tok_ref, grad_ref, logit_ref = held
    copies[0].wait()
    own_ref[...] = idx_ref[pl.ds(lax.axis_index("expert"), 1), :]
    experts, capacity = idx_ref.shape
    tok, cols = tok_ref.shape
    most = pick_ref.shape[0] // experts
    local = idx_ref[...] - lax.axis_index("expert") * tok
    mine = jnp.where((local >= 0) & (local < tok), 1.0, 0.0)
    before = (iota((capacity, capacity), 0) < iota((capacity, capacity), 1)).astype(f32)
    rank = mm(mine.astype(bf16), before.astype(bf16))
    rank = jnp.where(mine > 0.0, rank, -1.0)
    local = (local + 1).astype(f32)
    ranks = iota((most, capacity), 0).astype(f32)
    tokens = iota((most, tok), 1).astype(f32) + 1.0
    for e in range(experts):
        chosen = jnp.where(rank[e : e + 1] == ranks, local[e : e + 1], 0.0)
        chosen = jnp.sum(chosen, axis=1, keepdims=True)
        hit = jnp.where(chosen == tokens, 1.0, 0.0)
        pick_ref[e * most : (e + 1) * most, :] = hit.astype(bf16)
    pick = pick_ref[...]
    height = send_ref.shape[0] // experts
    at = 0
    for ref, copy in ((tok_ref, copies[1]), (grad_ref, copies[2])):
        copy.wait()
        rows = mm(pick, ref[...]).astype(bf16)
        for k in range(0, cols, LANES):
            for e in range(experts):
                to = e * height + at
                send_ref[to : to + most, :] = rows[e * most : (e + 1) * most, k : k + LANES]
            at += most
    copies[3].wait()
    rows = []
    for part in in_parts(logit_ref[...], 2):
        rows += [part[:, k : k + LANES] for k in range(0, tok, LANES)]
    extra = stacked_rows(rows, EXTRA).astype(bf16)
    for e in range(experts):
        to = e * height + at
        send_ref[to : to + SENT, :] = extra[e, :SENT]


def compact_kernel(own_ref, recv_ref, rows_ref, probs_ref, target_ref, got_ref, extra_ref, *, tok):
    capacity, spread = rows_ref.shape[0], got_ref.shape[0]
    sources = extra_ref.shape[1]
    most = spread // sources
    square = (capacity, capacity)
    own_row = own_ref[...]
    own_col = row_to_column(own_row)
    key_row = own_row // tok * capacity + iota((1, capacity), 1)
    key_col = own_col // tok * capacity + iota((capacity, 1), 0)
    pos_row = jnp.sum((key_col < key_row).astype(i32), axis=0, keepdims=True)
    token = jnp.sum(jnp.where(pos_row == iota(square, 0), own_row, 0), axis=1, keepdims=True)
    src = token // tok
    local = token - src * tok
    wide = (capacity, LANES)
    start = jnp.sum((own_col < iota(wide, 1) * tok).astype(i32), axis=0, keepdims=True)
    first = jnp.sum(jnp.where(src == iota(wide, 1), start, 0), axis=1, keepdims=True)
    target = src * most + iota((capacity, 1), 0) - first
    place = jnp.where(target == iota((capacity, spread), 1), 1.0, 0.0).astype(bf16)
    target_ref[...] = jnp.broadcast_to(target, wide)
    pick = jnp.where(src == iota((capacity, sources), 1), 1.0, 0.0).astype(bf16)
    height = recv_ref.shape[0] // sources
    blocks = rows_ref.shape[1] // LANES
    for e in range(sources):
        for k in range(blocks):
            at = e * height + k * most
            got_ref[e * most : (e + 1) * most, k * LANES : (k + 1) * LANES] = recv_ref[
                at : at + most, :
            ]
        extra = recv_ref[e * height + blocks * most : (e + 1) * height, :].astype(f32)
        for k in range(SENT):
            extra_ref[k, e : e + 1, :] = extra[k : k + 1]
    rows_ref[...] = mm(place, got_ref[...]).astype(bf16)
    lanes = iota(wide, 1)
    per = SENT // 2
    logits = jnp.zeros((capacity, 1), f32)
    for k in range(per):
        table = mm(pick, extra_ref[k].astype(bf16)) + mm(pick, extra_ref[per + k].astype(bf16))
        hit = lanes + k * LANES == local
        logits = logits + jnp.sum(jnp.where(hit, table, 0.0), axis=1, keepdims=True)
    probs_ref[...] = jax.nn.sigmoid(jnp.broadcast_to(logits, (capacity, LANES)))


def spans(ref, dim, offsets, devices):
    size = ref.shape[dim] // devices
    out = []
    for offset in offsets:
        block = lax.rem(lax.axis_index("mp") + offset + devices, devices)
        out.append(pl.ds(pl.multiple_of(block * size, size), size))
    return out


def pre_products(chunks, offsets, win_ref, devices):
    cols = win_ref.shape[0] // devices
    at = spans(win_ref, 0, offsets, devices)
    return sum(mm(chunk[:, :cols], win_ref[span, :]) for chunk, span in zip(chunks, at))


def back_products(chunks, offsets, wout_ref, devices):
    cols = wout_ref.shape[1] // devices
    at = spans(wout_ref, 1, offsets, devices)
    return sum(mm(chunk[:, cols:], wout_ref[:, span], ((1,), (1,))) for chunk, span in zip(chunks, at))


def first_kernel(*refs, offsets, devices):
    chunks, refs = refs[: len(offsets)], refs[len(offsets) :]
    target_ref, stored, (pre_ref, back_ref, place_ref), held, done = (
        refs[0], refs[1:3], refs[3:6], refs[6:8], refs[8]
    )
    copies = [pltpu.make_async_copy(a, b, done.at[k]) for k, (a, b) in enumerate(zip(stored, held))]
    for copy in copies:
        copy.start()
    target = column_to_row(target_ref[:, :1])
    place = jnp.where(target == iota(place_ref.shape, 0), 1.0, 0.0)
    place_ref[...] = place.astype(bf16)
    copies[0].wait()
    pre_ref[...] = pre_products(chunks, offsets, held[0], devices)
    copies[1].wait()
    back_ref[...] = back_products(chunks, offsets, held[1], devices)


def hidden_kernel(pre_ref, back_ref, *refs, offsets):
    chunks = refs[: len(offsets)]
    win_ref, wout_ref, out_ref = refs[len(offsets) :]
    devices = out_ref.shape[0]
    capacity, both = chunks[0].shape
    cols = both // 2
    pre = pre_ref[...] + pre_products(chunks, offsets, win_ref, devices)
    back = back_ref[...] + back_products(chunks, offsets, wout_ref, devices)
    cumulative = 0.5 * (1.0 + lax.erf(pre * inv_root_two))
    slopes = cumulative + pre * jnp.exp(-0.5 * pre * pre) * inv_root_tau
    gates = jnp.sum(pre * cumulative * back, axis=1, keepdims=True)
    delta = (back * slopes).astype(bf16)
    for d in range(devices):
        block = mm(delta, win_ref[d * cols : (d + 1) * cols, :], ((1,), (1,))).astype(bf16)
        for k in range(cols // LANES):
            out_ref[d, k * capacity : (k + 1) * capacity, :] = block[:, k * LANES : (k + 1) * LANES]
    gates = column_to_row(gates)
    rows = []
    for part in in_parts(gates, 3):
        rows += [part[:, k : k + LANES] for k in range(0, capacity, LANES)]
    extra = stacked_rows(rows, EXTRA).astype(bf16)
    at = cols // LANES * capacity
    out_ref[:, at : at + EXTRA, :] = jnp.broadcast_to(extra, (devices, EXTRA, LANES))


def combine_kernel(parts_ref, probs_ref, own_ref, router_ref, place_ref, out_ref):
    devices = parts_ref.shape[0]
    capacity, both = own_ref.shape
    cols = both // 2
    blocks = cols // LANES
    sources = router_ref.shape[0]
    most = place_ref.shape[0] // sources
    height = out_ref.shape[0] // sources
    at = blocks * capacity
    extra = jnp.sum(parts_ref[:, at : at + EXTRA, :].astype(f32), axis=0)
    per = capacity // LANES
    gates = extra[:per] + extra[per : 2 * per] + extra[2 * per : 3 * per]
    gates = jnp.concatenate([row_to_column(gates[k : k + 1]) for k in range(per)], axis=0)
    probs = probs_ref[...]
    logit_grad = (probs * (1.0 - probs) * gates).astype(bf16).astype(f32)
    router = router_ref[...].astype(f32)
    mine = iota(router.shape, 0) == lax.axis_index("expert")
    router = jnp.sum(jnp.where(mine, router, 0.0), axis=0, keepdims=True)
    rows, own = [], own_ref[:, :cols].astype(f32)
    for k in range(blocks):
        total = jnp.zeros((capacity, LANES), f32)
        for d in range(devices):
            total = total + parts_ref[d, k * capacity : (k + 1) * capacity, :].astype(f32)
        cut = slice(k * LANES, (k + 1) * LANES)
        block = (total * probs + logit_grad * router[:, cut]).astype(bf16)
        block = mm(place_ref[...], block).astype(bf16)
        for e in range(sources):
            to = e * height + k * most
            out_ref[to : to + most, :] = block[e * most : (e + 1) * most]
        rows.append(jnp.sum(own[:, cut] * logit_grad, axis=0, keepdims=True))
    extra = stacked_rows(rows, EXTRA).astype(bf16)
    for e in range(sources):
        out_ref[(e + 1) * height - BACK : (e + 1) * height, :] = extra[0, :BACK]


def finish_kernel(recv_ref, pick_ref, grad_ref, router_ref, got_ref):
    experts = router_ref.shape[0]
    most = pick_ref.shape[0] // experts
    height = recv_ref.shape[0] // experts
    blocks = grad_ref.shape[1] // LANES
    for e in range(experts):
        extra = recv_ref[(e + 1) * height - BACK : (e + 1) * height, :].astype(f32)
        for k in range(blocks):
            cut = slice(k * LANES, (k + 1) * LANES)
            at = e * height + k * most
            got_ref[e * most : (e + 1) * most, cut] = recv_ref[at : at + most, :]
            router_ref[e : e + 1, cut] = extra[k : k + 1]
    grad_ref[...] = mm(pick_ref[...], got_ref[...], ((0,), (0,)))


def exchanged(x, axis):
    shape = (lax.axis_size(axis), -1, 2, LANES)
    return lax.all_to_all(x.reshape(shape), axis, 0, 0, tiled=True).reshape(x.shape)


def kernel_call(body, outs, scalars, *args, flops=0, hbm=0, scratch=()):
    vmem = pl.BlockSpec(memory_space=pltpu.VMEM)
    smem = pl.BlockSpec(memory_space=pltpu.SMEM)
    far = pl.BlockSpec(memory_space=pltpu.HBM)
    shapes = [jax.ShapeDtypeStruct(s, t) for s, t in outs]
    near = len(args) - hbm
    args = args[:near] + tuple(pltpu.with_memory_space_constraint(x, pltpu.HBM) for x in args[near:])
    return pl.pallas_call(
        body,
        out_shape=shapes,
        in_specs=[smem] * scalars + [vmem] * (near - scalars) + [far] * hbm,
        out_specs=[vmem] * len(shapes),
        scratch_shapes=list(scratch),
        cost_estimate=pl.CostEstimate(flops=flops, transcendentals=0, bytes_accessed=0) if flops else None,
        compiler_params=pltpu.CompilerParams(vmem_limit_bytes=SCOPED),
    )(*args)


def ring_gather(x, axis):
    n = lax.axis_size(axis)
    up = [(k, (k + 1) % n) for k in range(n)]
    down = [(k, (k - 1) % n) for k in range(n)]
    chunks, offsets = [x], [0]
    right = left = x
    for step in range(1, n // 2 + 1):
        right = lax.ppermute(right, axis, up)
        chunks.append(right)
        offsets.append(-step)
        if 2 * step < n:
            left = lax.ppermute(left, axis, down)
            chunks.append(left)
            offsets.append(step)
    return chunks, tuple(offsets)


def per_device(tokens_in, out_grad, logits, indices, w_in, w_out, router_w):
    tok, cols = tokens_in.shape
    experts, capacity = indices.shape
    most = min(tok, 2 * capacity // experts)
    spread = experts * most
    devices = lax.axis_size("mp")
    blocks = cols // LANES
    given = (indices, tokens_in, out_grad, logits.T)
    send, pick, own = kernel_call(
        pack_kernel,
        [
            ((experts * (2 * blocks * most + SENT), LANES), bf16),
            ((spread, tok), bf16),
            ((1, capacity), i32),
        ],
        0,
        *given,
        hbm=4,
        scratch=[pltpu.VMEM(x.shape, x.dtype) for x in given] + [pltpu.SemaphoreType.DMA((4,))],
    )
    recv = exchanged(send, "expert")
    rows, probs, target = kernel_call(
        functools.partial(compact_kernel, tok=tok),
        [((capacity, 2 * cols), bf16), ((capacity, LANES), f32), ((capacity, LANES), i32)],
        0,
        own,
        recv,
        scratch=[pltpu.VMEM((spread, 2 * cols), bf16), pltpu.VMEM((SENT, experts, LANES), f32)],
    )
    chunks, offsets = ring_gather(rows, "mp")
    hidden = w_in.shape[2]
    early = len(chunks) - 1
    pre, back, place_back, win, wout = kernel_call(
        functools.partial(first_kernel, offsets=offsets[:early], devices=devices),
        [((capacity, hidden), f32)] * 2
        + [((spread, capacity), bf16), (w_in.shape[1:], bf16), (w_out.shape[1:], bf16)],
        0,
        *chunks[:early],
        target,
        w_in[0],
        w_out[0],
        hbm=2,
        scratch=[pltpu.SemaphoreType.DMA((2,))],
        flops=4 * early * capacity * cols * hidden,
    )
    (parts,) = kernel_call(
        functools.partial(hidden_kernel, offsets=offsets[early:]),
        [((devices, blocks * capacity + EXTRA, LANES), bf16)],
        0,
        pre,
        back,
        *chunks[early:],
        win,
        wout,
    )
    parts = lax.all_to_all(parts, "mp", 0, 0, tiled=True)
    (back,) = kernel_call(
        combine_kernel,
        [((experts * (blocks * most + BACK), LANES), bf16)],
        0,
        parts,
        probs,
        rows,
        router_w.T,
        place_back,
    )
    back = exchanged(back, "expert")
    input_grad, router_grad = kernel_call(
        finish_kernel,
        [((tok, cols), f32), ((experts, cols), f32)],
        0,
        back,
        pick,
        scratch=[pltpu.VMEM((spread, cols), bf16)],
    )
    return input_grad, router_grad.T


def solution(mesh):
    return jax.shard_map(
        per_device,
        mesh=mesh,
        in_specs=(
            P(("groups", "expert"), "mp"),
            P(("groups", "expert"), "mp"),
            P(("groups", "expert"), None),
            P("groups", None),
            P("expert", None, "mp"),
            P("expert", "mp", None),
            P("mp", None),
        ),
        out_specs=(P(("groups", "expert"), "mp"), P(("groups", "mp"), None)),
        check_vma=False,
    )
```
